16 devices in a mesh: dp: 4 (over z, y), tp: 4 (over x, core).
Axes of the slice: x: 2, y: 2, z: 2, core: 2. Of those that a mesh axis runs over, the one named last changes fastest.
Arguments:
- hidden_in: bfloat16 [128, 2048], P('dp'), parts along dimension 0
- k_cache: bfloat16 [128, 256, 16, 128], P('dp', None, 'tp'), parts along dimension 0
- v_cache: bfloat16 [128, 256, 16, 128], P('dp', None, 'tp'), parts along dimension 0
- seq_lens: int32 [128], P('dp'), parts along dimension 0
- chosen_experts: int32 [128, 4], P('dp'), parts along dimension 0
- g_attn: bfloat16 [2048], replicated
- w_q: bfloat16 [2048, 2048], P(None, 'tp')
- w_k: bfloat16 [2048, 2048], P(None, 'tp')
- w_v: bfloat16 [2048, 2048], P(None, 'tp')
- w_o: bfloat16 [2048, 2048], P('tp')
- g_moe: bfloat16 [2048], replicated
- w_router: bfloat16 [2048, 60], replicated
- w_gate: bfloat16 [60, 2048, 1408], P(None, None, 'tp')
- w_up: bfloat16 [60, 2048, 1408], P(None, None, 'tp')
- w_down: bfloat16 [60, 1408, 2048], P(None, 'tp')
Outputs:
- output 1: bfloat16 [128, 2048], P('dp'), parts along dimension 0
- output 2: bfloat16 [128, 256, 16, 128], P('dp', None, 'tp'), parts along dimension 0
- output 3: bfloat16 [128, 256, 16, 128], P('dp', None, 'tp'), parts along dimension 0
There are 4 independent parts. The reference program is written for one: setup_inputs(seed, part) draws one part's arguments, and reference() takes and returns one part's arrays. A program takes and returns all parts, laid end to end along the dimension named above; an argument that names none is the same for every part.
All inputs are finite; a program needn't handle non-finite values.
Results may differ from the reference program's by a relative error of at most 0.0140183.
Values are sent between devices in bfloat16 or wider.
A program may use at most 1.25 GiB of HBM per device.

```python
import math
import jax
import jax.numpy as jnp
from jax import lax

BATCH_SEQS = 32
CACHE_LEN = 256
D_MODEL = 2048
Q_HEADS = 16
KV_HEADS = 16
HEAD_DIM = 128
FFN_DIM = 1408
EXPERTS = 60
TOP_K = 4


def draw_layout(len_key, pick_key):
    seq_lens = jax.random.randint(len_key, (BATCH_SEQS,), 1, CACHE_LEN, dtype=jnp.int32)
    seq_lens = seq_lens.at[0].set(CACHE_LEN - 1)
    expert_ids = jnp.arange(EXPERTS, dtype=jnp.int32)
    hot_bonus = jnp.where(expert_ids < max(1, EXPERTS // 8), 2 * EXPERTS, 0)
    end_bonus = jnp.where((expert_ids == 0) | (expert_ids == EXPERTS - 1), 16 * EXPERTS, 0)
    first_row = (jnp.arange(BATCH_SEQS) == 0)[:, None]
    scores = jax.random.randint(pick_key, (BATCH_SEQS, EXPERTS), 0, 4 * EXPERTS, dtype=jnp.int32)
    scores = scores + hot_bonus[None, :] + jnp.where(first_row, end_bonus[None, :], 0)
    _, chosen_ids = lax.top_k(scores * EXPERTS + expert_ids[None, :], TOP_K)
    return seq_lens, chosen_ids.astype(jnp.int32)


def normal_weight(rng_key, out_shape, fan_in, factor):
    return (factor * fan_in ** -0.5 * jax.random.normal(rng_key, out_shape, jnp.float32)).astype(jnp.bfloat16)


def setup_inputs(seed: int = 0, part: int = 0) -> dict:
    part_keys = jax.random.split(jax.random.fold_in(jax.random.key(seed), part), 5)
    shared = jax.random.split(jax.random.key(seed + 1), 12)
    q_width = Q_HEADS * HEAD_DIM
    kv_width = KV_HEADS * HEAD_DIM
    key_scale = math.sqrt(0.75 * math.log(CACHE_LEN))
    cache_shape = (BATCH_SEQS, CACHE_LEN, KV_HEADS, HEAD_DIM)
    seq_lens, chosen_experts = draw_layout(part_keys[3], part_keys[4])
    return {
        "hidden_in": jax.random.normal(part_keys[0], (BATCH_SEQS, D_MODEL), jnp.float32).astype(jnp.bfloat16),
        "k_cache": (key_scale * jax.random.normal(part_keys[1], cache_shape, jnp.float32)).astype(jnp.bfloat16),
        "v_cache": jax.random.normal(part_keys[2], cache_shape, jnp.float32).astype(jnp.bfloat16),
        "seq_lens": seq_lens,
        "chosen_experts": chosen_experts,
        "g_attn": jax.random.uniform(shared[0], (D_MODEL,), jnp.float32, 0.5, 1.5).astype(jnp.bfloat16),
        "w_q": normal_weight(shared[1], (D_MODEL, q_width), D_MODEL, 1.0),
        "w_k": normal_weight(shared[2], (D_MODEL, kv_width), D_MODEL, 1.0),
        "w_v": normal_weight(shared[3], (D_MODEL, kv_width), D_MODEL, 1.0),
        "w_o": normal_weight(shared[4], (q_width, D_MODEL), q_width, 2.0),
        "g_moe": jax.random.uniform(shared[5], (D_MODEL,), jnp.float32, 0.5, 1.5).astype(jnp.bfloat16),
        "w_router": normal_weight(shared[6], (D_MODEL, EXPERTS), D_MODEL, 1.0),
        "w_gate": normal_weight(shared[7], (EXPERTS, D_MODEL, FFN_DIM), D_MODEL, 1.0),
        "w_up": normal_weight(shared[8], (EXPERTS, D_MODEL, FFN_DIM), D_MODEL, 1.0),
        "w_down": normal_weight(shared[9], (EXPERTS, FFN_DIM, D_MODEL), FFN_DIM, 2.0 * math.sqrt(TOP_K)),
    }


def rms_norm(vector, gain_w):
    vector32 = vector.astype(jnp.float32)
    norm_scale = lax.rsqrt(jnp.mean(vector32 * vector32, axis=-1, keepdims=True) + 1e-5)
    return (vector32 * norm_scale * gain_w.astype(jnp.float32)).astype(jnp.bfloat16)


def rope_rotate(vector, cos_t, sin_t):
    half_dim = vector.shape[-1] // 2
    lead_half = vector[..., :half_dim]
    tail_half = vector[..., half_dim:]
    return jnp.concatenate([lead_half * cos_t - tail_half * sin_t, tail_half * cos_t + lead_half * sin_t], axis=-1)


def attend_one(operands):
    q_seq, k_seq, v_seq, seq_len = operands
    scores = jnp.einsum("kgd,skd->kgs", q_seq.astype(jnp.float32), k_seq.astype(jnp.float32)) * HEAD_DIM ** -0.5
    in_range = (jnp.arange(CACHE_LEN) <= seq_len)[None, None, :]
    attn_weights = jax.nn.softmax(jnp.where(in_range, scores, -1e30), axis=-1).astype(jnp.bfloat16)
    return jnp.einsum("kgs,skd->kgd", attn_weights.astype(jnp.float32), v_seq.astype(jnp.float32)).astype(jnp.bfloat16)


def reference(hidden_in, k_cache, v_cache, seq_lens, chosen_experts, g_attn, w_q, w_k, w_v, w_o, g_moe, w_router, w_gate, w_up, w_down):
    q_group = Q_HEADS // KV_HEADS
    h_attn = rms_norm(hidden_in, g_attn)
    q_lin = jnp.dot(h_attn, w_q, preferred_element_type=jnp.float32).reshape(BATCH_SEQS, KV_HEADS, q_group, HEAD_DIM)
    k_lin = jnp.dot(h_attn, w_k, preferred_element_type=jnp.float32).reshape(BATCH_SEQS, KV_HEADS, HEAD_DIM)
    v_new = jnp.dot(h_attn, w_v, preferred_element_type=jnp.float32).reshape(BATCH_SEQS, KV_HEADS, HEAD_DIM).astype(jnp.bfloat16)
    inv_freq = 1000000.0 ** (-jnp.arange(0, HEAD_DIM, 2, dtype=jnp.float32) / HEAD_DIM)
    angles = seq_lens.astype(jnp.float32)[:, None] * inv_freq[None, :]
    cos_t = jnp.cos(angles)[:, None, :]
    sin_t = jnp.sin(angles)[:, None, :]
    q_rot = rope_rotate(q_lin, cos_t[:, :, None, :], sin_t[:, :, None, :]).astype(jnp.bfloat16)
    k_new = rope_rotate(k_lin, cos_t, sin_t).astype(jnp.bfloat16)
    new_slot = (jnp.arange(CACHE_LEN)[None, :] == seq_lens[:, None])[:, :, None, None]
    k_next = jnp.where(new_slot, k_new[:, None, :, :], k_cache)
    v_next = jnp.where(new_slot, v_new[:, None, :, :], v_cache)
    heads_out = lax.map(attend_one, (q_rot, k_next, v_next, seq_lens))
    attn_sum = jnp.dot(heads_out.reshape(BATCH_SEQS, Q_HEADS * HEAD_DIM), w_o, preferred_element_type=jnp.float32)
    hidden_mid = (hidden_in.astype(jnp.float32) + attn_sum).astype(jnp.bfloat16)
    h_moe = rms_norm(hidden_mid, g_moe)
    logits = jnp.dot(h_moe, w_router, preferred_element_type=jnp.float32)
    pick_mask = (chosen_experts[:, :, None] == jnp.arange(EXPERTS)[None, None, :]).astype(jnp.float32)
    gate_probs = jax.nn.softmax(jnp.sum(pick_mask * logits[:, None, :], axis=-1), axis=-1)
    gate_mat = jnp.sum(gate_probs[:, :, None] * pick_mask, axis=1)

    def expert_step(running, operands):
        gate_w, up_w, down_w, gate_col = operands
        up_gate = jnp.dot(h_moe, gate_w, preferred_element_type=jnp.float32)
        up_lin = jnp.dot(h_moe, up_w, preferred_element_type=jnp.float32)
        inner_act = (gate_col[:, None] * jax.nn.silu(up_gate) * up_lin).astype(jnp.bfloat16)
        return running + jnp.dot(inner_act, down_w, preferred_element_type=jnp.float32), None

    moe_sum, _ = lax.scan(expert_step, jnp.zeros((BATCH_SEQS, D_MODEL), jnp.float32), (w_gate, w_up, w_down, gate_mat.T))
    hidden_out = (hidden_mid.astype(jnp.float32) + moe_sum).astype(jnp.bfloat16)
    return (hidden_out, k_next, v_next)
```

```python
import functools
import jax
import jax.numpy as jnp
from jax import lax
from jax.experimental import pallas as pl
from jax.experimental.pallas import tpu as pltpu
from jax.sharding import PartitionSpec as P

EPSILON = 1e-5
ROPE_THETA = 1000000.0
MASK_FILL = -1e30
MESH = pl.DeviceIdType.MESH
F32 = jnp.float32
BF16 = jnp.bfloat16
NT = (((1,), (1,)), ((), ()))
ANY = pl.BlockSpec(memory_space=pl.ANY)
VMEM = pl.BlockSpec(memory_space=pltpu.VMEM)
SMEM = pl.BlockSpec(memory_space=pltpu.SMEM)


def norm_rows(x32, gain):
    scale = lax.rsqrt(jnp.mean(x32 * x32, axis=-1, keepdims=True) + EPSILON)
    return (x32 * scale * gain.astype(F32)).astype(BF16)


def attention_kernel(lens, x_ref, g_ref, freq_ref, wq, wk, wv, wo, kc, vc, part_ref, kout, vout,
                     kbuf, vbuf, qkvw, wobuf, qs, ks, vs, os_, wsem, insem, outsem, *, group):
    rows = x_ref.shape[0]
    heads = wq.shape[1] // 128
    slots = kc.shape[1]
    steps = rows // group
    wcopies = [pltpu.make_async_copy(w, qkvw.at[i], wsem.at[i]) for i, w in enumerate((wq, wk, wv))]
    wocopy = pltpu.make_async_copy(wo, wobuf, wsem.at[3])
    for cp in wcopies:
        cp.start()

    def fetch(i, hbm, buf, j):
        at = pl.ds(i * group, group)
        return pltpu.make_async_copy(hbm.at[at], buf.at[at], insem.at[j, i])

    def flush(i, hbm, buf, j):
        at = pl.ds(i * group, group)
        return pltpu.make_async_copy(buf.at[at], hbm.at[at], outsem.at[j, i])

    for i in range(steps):
        fetch(i, kc, kbuf, 0).start()
        fetch(i, vc, vbuf, 1).start()
    wocopy.start()

    h = norm_rows(x_ref[...].astype(F32), g_ref[...])
    row_id = lax.broadcasted_iota(jnp.int32, (rows, 128), 0)
    pos = jnp.zeros((rows, 128), jnp.int32)
    for b in range(rows):
        pos = jnp.where(row_id == b, lens[b], pos)
    ang = pos.astype(F32) * freq_ref[...]
    cos_t = jnp.cos(ang)
    sin_t = jnp.sin(ang)
    lane = lax.broadcasted_iota(jnp.int32, (rows, 128), 1)
    sin_t = jnp.where(lane < 64, -sin_t, sin_t)

    def rope(u):
        return u * cos_t + pltpu.roll(u, 64, 1) * sin_t

    wcopies[0].wait()
    q = jnp.dot(h, qkvw[0], preferred_element_type=F32)
    wcopies[1].wait()
    k = jnp.dot(h, qkvw[1], preferred_element_type=F32)
    wcopies[2].wait()
    v = jnp.dot(h, qkvw[2], preferred_element_type=F32)
    for j in range(heads):
        cols = slice(128 * j, 128 * j + 128)
        qs[pl.ds(j, rows, stride=heads), :] = rope(q[:, cols]).astype(BF16).astype(F32)
        kj = rope(k[:, cols]).astype(BF16).astype(F32)
        vj = v[:, cols].astype(BF16).astype(F32)
        for rep in range(8 // heads):
            ks[pl.ds(j + rep * heads, rows, stride=8), :] = kj
            vs[pl.ds(j + rep * heads, rows, stride=8), :] = vj

    qrows = group * heads
    rid = lax.broadcasted_iota(jnp.int32, (qrows, slots), 0)
    cid = lax.broadcasted_iota(jnp.int32, (qrows, slots), 1)
    same_head = lax.rem(rid, heads) == lax.rem(cid, heads)
    slot = lax.div(cid, heads)
    seq_of = lax.div(rid, heads)
    oseq = lax.div(lax.broadcasted_iota(jnp.int32, (qrows, 128), 0), heads)
    trow = lax.div(lax.broadcasted_iota(jnp.int32, (16, 128), 0), heads)

    def insert(buf, new, b, p):
        at = pl.ds(pl.multiple_of(lax.div(p * heads, 16) * 16, 16), 16)
        n8 = new[pl.ds(pl.multiple_of(b * 8, 8), 8), :]
        n16 = jnp.concatenate([n8, n8], axis=0)
        old = buf[b, at, :].astype(F32)
        buf[b, at, :] = jnp.where(trow == lax.rem(p, 16 // heads), n16, old).astype(BF16)

    def step(i, carry):
        q16 = qs[pl.ds(pl.multiple_of(i * qrows, qrows), qrows), :].astype(BF16)
        fetch(i, kc, kbuf, 0).wait()
        ps = [lens[i * group + u] for u in range(group)]
        for u in range(group):
            insert(kbuf, ks, i * group + u, ps[u])
        flush(i, kout, kbuf, 0).start()
        sc = jnp.zeros((qrows, slots), F32)
        pm = jnp.zeros((qrows, slots), jnp.int32)
        for u in range(group):
            s_u = lax.dot_general(q16, kbuf[i * group + u], NT, preferred_element_type=F32)
            sc = jnp.where(seq_of == u, s_u, sc)
            pm = jnp.where(seq_of == u, ps[u], pm)
        sc = jnp.where(same_head & (slot <= pm), sc * (128 ** -0.5), MASK_FILL)
        ex = jnp.exp(sc - jnp.max(sc, axis=-1, keepdims=True))
        wt = (ex / jnp.sum(ex, axis=-1, keepdims=True)).astype(BF16)
        fetch(i, vc, vbuf, 1).wait()
        for u in range(group):
            insert(vbuf, vs, i * group + u, ps[u])
        flush(i, vout, vbuf, 1).start()
        o = jnp.zeros((qrows, 128), F32)
        for u in range(group):
            o_u = jnp.dot(wt, vbuf[i * group + u], preferred_element_type=F32)
            o = jnp.where(oseq == u, o_u, o)
        os_[pl.ds(pl.multiple_of(i * qrows, qrows), qrows), :] = o
        return carry

    lax.fori_loop(0, steps, step, 0)
    o = jnp.concatenate([os_[pl.ds(j, rows, stride=heads), :] for j in range(heads)], axis=1).astype(BF16)
    wocopy.wait()
    part_ref[...] = jnp.dot(o, wobuf[...], preferred_element_type=F32)

    def drain(i, carry):
        flush(i, kout, kbuf, 0).wait()
        flush(i, vout, vbuf, 1).wait()
        return carry

    lax.fori_loop(0, steps, drain, 0)


def attention(x, kc, vc, lens, g, wq, wk, wv, wo):
    rows, d_model = x.shape
    _, slots, _ = kc.shape
    width = wq.shape[1]
    heads = width // 128
    group = 4
    steps = rows // group
    freq = ROPE_THETA ** (-jnp.arange(0, 128, 2, dtype=F32) / 128)
    freq = jnp.concatenate([freq, freq])[None, :]
    return pl.pallas_call(
        functools.partial(attention_kernel, group=group),
        name="attention",
        out_shape=(jax.ShapeDtypeStruct((rows, d_model), F32),
                   jax.ShapeDtypeStruct(kc.shape, BF16), jax.ShapeDtypeStruct(vc.shape, BF16)),
        in_specs=[SMEM, VMEM, VMEM, VMEM, ANY, ANY, ANY, ANY, ANY, ANY],
        out_specs=(VMEM, ANY, ANY),
        scratch_shapes=[
            pltpu.VMEM((rows, slots, 128), BF16),
            pltpu.VMEM((rows, slots, 128), BF16),
            pltpu.VMEM((3, d_model, width), BF16),
            pltpu.VMEM((width, d_model), BF16),
            pltpu.VMEM((rows * heads, 128), F32),
            pltpu.VMEM((rows * 8, 128), F32),
            pltpu.VMEM((rows * 8, 128), F32),
            pltpu.VMEM((rows * heads, 128), F32),
            pltpu.SemaphoreType.DMA((4,)),
            pltpu.SemaphoreType.DMA((2, steps)),
            pltpu.SemaphoreType.DMA((2, steps)),
        ],
        compiler_params=pltpu.CompilerParams(vmem_limit_bytes=63 << 20),
        cost_estimate=pl.CostEstimate(flops=400_000_000, bytes_accessed=42_000_000, transcendentals=0),
    )(lens, x, g[None, :], freq, wq, wk, wv, wo, kc, vc)


def experts_kernel(part, x_ref, g_ref, picks, wr, wg, wu, wd, out_ref,
                   gbuf, ubuf, dbuf, xf, recv1, hall, hb, gall, z, acc, drecv, psum, frecv, yall,
                   gsem, usem, dsem, s1, r1, s2, r2, s3, r3, s4, r4, s5, r5, s6, r6, s7, r7, s8, r8,
                   *, n_dp, n_tp, ring, chunks):
    dp = lax.axis_index("dp")
    tp = lax.axis_index("tp")
    core = lax.rem(tp, 2)
    xx = lax.div(tp, 2)
    n_exp, f_dim, d_model = wg.shape
    mine = n_exp // n_dp
    base = dp * mine
    f_pad = z.shape[1] // mine
    n_chip = n_dp * n_tp // 2
    me_chip = dp * (n_tp // 2) + xx
    me = dp * n_tp + tp
    n_blk = n_dp * n_tp
    rows = x_ref.shape[0]
    cw = d_model // chunks

    def flip(v, bit):
        return 1 - v if bit else v

    def chip_peer(m):
        px = flip(xx, m & 1)
        pd = 2 * flip(lax.div(dp, 2), (m >> 2) & 1) + flip(lax.rem(dp, 2), (m >> 1) & 1)
        return pd, px

    peers = []
    for m in range(1, n_chip):
        pd, px = chip_peer(m)
        peers.append({"dp": pd, "tp": 2 * px + core})
    partner = {"dp": dp, "tp": 2 * xx + 1 - core}
    cross = {"dp": dp, "tp": 2 * (1 - xx) + 1 - core}

    def gcopy(e, s):
        return pltpu.make_async_copy(wg.at[base + e], gbuf.at[s], gsem.at[s])

    def ucopy(e, s):
        return pltpu.make_async_copy(wu.at[base + e], ubuf.at[s], usem.at[s])

    def dcopy(e):
        return pltpu.make_async_copy(wd.at[base + e], dbuf.at[pl.ds(e * f_pad, f_dim)], dsem.at[e])

    barrier = pltpu.get_barrier_semaphore()
    for dev in peers + [partner, cross]:
        pl.semaphore_signal(barrier, inc=1, device_id=dev, device_id_type=MESH)
    for e in range(ring):
        gcopy(e, e).start()
        ucopy(e, e).start()
    for e in range(mine):
        dcopy(e).start()
    xf[...] = x_ref[...].astype(F32)
    pl.semaphore_wait(barrier, len(peers) + 2)

    def block(t):
        return pl.ds(pl.multiple_of(t * 8, 8), 8)

    first = []
    for k in range(1, n_tp):
        t_to = lax.rem(tp + k, n_tp)
        cp = pltpu.make_async_remote_copy(
            src_ref=part.at[block(t_to)], dst_ref=recv1.at[k - 1],
            send_sem=s1.at[k - 1], recv_sem=r1.at[k - 1],
            device_id={"dp": dp, "tp": t_to}, device_id_type=MESH)
        cp.start()
        first.append(cp)

    for e in range(mine):
        dbuf[pl.ds(e * f_pad + f_dim, f_pad - f_dim), :] = jnp.zeros((f_pad - f_dim, d_model), BF16)
    z[...] = jnp.zeros_like(z)
    pick_cols = []
    row8 = lax.broadcasted_iota(jnp.int32, (8, 128), 0)
    for kk in range(picks.shape[0]):
        pc = jnp.zeros((8, 128), jnp.int32)
        for i in range(8):
            pc = jnp.where(row8 == i, picks[kk, tp * 8 + i], pc)
        pick_cols.append(pc)

    for cp in first:
        cp.wait()
    attn_sum = part[block(tp), :]
    for k in range(1, n_tp):
        attn_sum = attn_sum + recv1[k - 1]
    x1 = (xf[block(tp), :] + attn_sum).astype(BF16).astype(F32)
    xf[block(tp), :] = x1
    h2 = norm_rows(x1, g_ref[...])
    hall[me] = h2

    def spread(buf, i, m, ssem, rsem):
        return pltpu.make_async_remote_copy(
            src_ref=buf.at[i], dst_ref=buf.at[i], send_sem=ssem.at[m], recv_sem=rsem.at[m],
            device_id=peers[m], device_id_type=MESH)

    def relay(buf, i, m, ssem, rsem):
        return pltpu.make_async_remote_copy(
            src_ref=buf.at[i], dst_ref=buf.at[i], send_sem=ssem.at[m], recv_sem=rsem.at[m],
            device_id=partner, device_id_type=MESH)

    order = sorted(range(n_chip - 1), key=lambda m: -bin(m + 1).count("1"))
    hs = [spread(hall, me, m, s2, r2) for m in range(n_chip - 1)]
    hd = [relay(hall, me, n_chip - 1, s3, r3)]
    for m in order:
        hs[m].start()
    hd[0].start()

    logits = lax.dot_general(h2, wr[...], NT, preferred_element_type=F32)
    lane = lax.broadcasted_iota(jnp.int32, (8, 128), 1)
    picked = []
    for pc in pick_cols:
        hit = (lane == pc)[:, :n_exp]
        picked.append(jnp.sum(jnp.where(hit, logits, 0.0), axis=1, keepdims=True))
    top = functools.reduce(jnp.maximum, picked)
    exs = [jnp.exp(p - top) for p in picked]
    den = functools.reduce(lambda a, b: a + b, exs)
    gates = jnp.zeros((8, 128), F32)
    for pc, ex in zip(pick_cols, exs):
        gates = gates + jnp.where(lane == pc, ex / den, 0.0)
    gall[me] = gates
    gs = [spread(gall, me, m, s4, r4) for m in range(n_chip - 1)]
    gd = [relay(gall, me, n_chip - 1, s5, r5)]
    for m in order:
        gs[m].start()
    gd[0].start()

    def owner(m):
        pd, px = chip_peer(m + 1)
        return pd * n_tp + 2 * px + core

    for m in reversed(order):
        hs[m].wait_recv()
        cp = relay(hall, owner(m), m, s3, r3)
        cp.start()
        hd.append(cp)
    for m in reversed(order):
        gs[m].wait_recv()
        cp = relay(gall, owner(m), m, s5, r5)
        cp.start()
        gd.append(cp)
    for cp in hd + gd:
        cp.wait_recv()
    for cp in hs + gs + hd + gd:
        cp.wait_send()

    for r in range(n_blk // 2):
        two = jnp.concatenate([hall[2 * r].astype(F32), hall[2 * r + 1].astype(F32)], axis=0)
        hb[16 * r:16 * r + 16, :] = two.astype(BF16)
    gmat = gall[...].reshape(n_blk * 8, 128)
    glane = lax.broadcasted_iota(jnp.int32, (n_blk * 8, 128), 1)

    def expert(e, s):
        gcopy(e, s).wait()
        ucopy(e, s).wait()
        gate = lax.dot_general(hb[...], gbuf[s], NT, preferred_element_type=F32)
        up = lax.dot_general(hb[...], ubuf[s], NT, preferred_element_type=F32)
        gcol = jnp.sum(jnp.where(glane == base + e, gmat, 0.0), axis=1, keepdims=True)
        return (gcol * (gate * jax.nn.sigmoid(gate)) * up).astype(BF16)

    unroll = 3
    for e0 in range(0, mine, unroll):
        for e in range(e0, e0 + unroll):
            s = e % ring
            z[:, e * f_pad:e * f_pad + f_dim] = expert(e, s)
            if e + ring < mine:
                gcopy(e + ring, s).start()
                ucopy(e + ring, s).start()

    for e in range(mine):
        dcopy(e).wait()

    pend = []
    finals = {}
    pair = {}

    def pair_sum(n):
        pair[n].wait_recv()
        psum[n] = acc[n, core] + drecv[n]
        for m in order:
            pd, px = chip_peer(m + 1)
            chip = pd * (n_tp // 2) + px
            cp = pltpu.make_async_remote_copy(
                src_ref=psum.at[n, block(chip)], dst_ref=frecv.at[n, m],
                send_sem=s7.at[n, m], recv_sem=r7.at[n, m], device_id=peers[m], device_id_type=MESH)
            cp.start()
            finals[n, m] = cp

    for n in range(chunks):
        res = jnp.dot(z[...], dbuf[:, n * cw:(n + 1) * cw], preferred_element_type=F32)
        for j in range(n_chip):
            for q in range(2):
                at = (2 * j + q) * 8
                acc[n, q, 8 * j:8 * j + 8, :] = res[at:at + 8, :]
        cp = pltpu.make_async_remote_copy(
            src_ref=acc.at[n, 1 - core], dst_ref=drecv.at[n], send_sem=s6.at[n], recv_sem=r6.at[n],
            device_id=partner, device_id_type=MESH)
        cp.start()
        pair[n] = cp
        if n >= 1:
            pair_sum(n - 1)
    pair_sum(chunks - 1)
    for n in range(chunks):
        total = psum[n, block(me_chip), :]
        for m in range(n_chip - 1):
            finals[n, m].wait_recv()
            total = total + frecv[n, m]
        cols = slice(n * cw, (n + 1) * cw)
        yall[tp, :, cols] = (xf[block(tp), cols] + total).astype(BF16)
    last = []
    for k in range(1, n_tp):
        t_to = lax.rem(tp + k, n_tp)
        cp = pltpu.make_async_remote_copy(
            src_ref=yall.at[tp], dst_ref=yall.at[tp], send_sem=s8.at[k - 1], recv_sem=r8.at[k - 1],
            device_id={"dp": dp, "tp": t_to}, device_id_type=MESH)
        cp.start()
        last.append(cp)
    for cp in last:
        cp.wait_recv()
    out_ref[...] = yall[...]
    for cp in last + list(pair.values()) + list(finals.values()):
        cp.wait_send()


def experts(part, x, picks, g, wr, wg, wu, wd, n_dp, n_tp):
    rows, d_model = x.shape
    n_exp, f_dim, _ = wg.shape
    mine = n_exp // n_dp
    f_pad = -(-f_dim // 128) * 128
    ring, chunks = 10, 4
    n_chip = n_dp * n_tp // 2
    cw = d_model // chunks
    dma = pltpu.SemaphoreType.DMA
    out = pl.pallas_call(
        functools.partial(experts_kernel, n_dp=n_dp, n_tp=n_tp, ring=ring, chunks=chunks),
        name="experts",
        out_shape=jax.ShapeDtypeStruct((n_tp, 8, d_model), BF16),
        in_specs=[VMEM, VMEM, VMEM, SMEM, VMEM, ANY, ANY, ANY],
        out_specs=VMEM,
        scratch_shapes=[
            pltpu.VMEM((ring, f_dim, d_model), BF16),
            pltpu.VMEM((ring, f_dim, d_model), BF16),
            pltpu.VMEM((mine * f_pad, d_model), BF16),
            pltpu.VMEM((rows, d_model), F32),
            pltpu.VMEM((n_tp - 1, 8, d_model), F32),
            pltpu.VMEM((n_dp * n_tp, 8, d_model), BF16),
            pltpu.VMEM((n_dp * n_tp * 8, d_model), BF16),
            pltpu.VMEM((n_dp * n_tp, 8, 128), F32),
            pltpu.VMEM((n_dp * n_tp * 8, mine * f_pad), BF16),
            pltpu.VMEM((chunks, 2, n_chip * 8, cw), F32),
            pltpu.VMEM((chunks, n_chip * 8, cw), F32),
            pltpu.VMEM((chunks, n_chip * 8, cw), F32),
            pltpu.VMEM((chunks, n_chip - 1, 8, cw), F32),
            pltpu.VMEM((n_tp, 8, d_model), BF16),
            dma((ring,)), dma((ring,)), dma((mine,)),
            dma((n_tp - 1,)), dma((n_tp - 1,)),
            dma((n_chip - 1,)), dma((n_chip - 1,)),
            dma((n_chip,)), dma((n_chip,)),
            dma((n_chip - 1,)), dma((n_chip - 1,)),
            dma((n_chip,)), dma((n_chip,)),
            dma((chunks,)), dma((chunks,)),
            dma((chunks, n_chip - 1)), dma((chunks, n_chip - 1)),
            dma((n_tp - 1,)), dma((n_tp - 1,)),
        ],
        compiler_params=pltpu.CompilerParams(
            collective_id=0, has_side_effects=True, vmem_limit_bytes=63 << 20),
        cost_estimate=pl.CostEstimate(flops=8_000_000_000, bytes_accessed=66_000_000, transcendentals=0),
    )(part, x, g[None, :], picks, wr, wg, wu, wd)
    return out.reshape(rows, d_model)


def solution(mesh):
    cache_spec = P("dp", None, "tp", None)
    in_specs = (P("dp", None), cache_spec, cache_spec, P("dp"), P("dp", None), P(None), P(None, "tp"), P(None, "tp"), P(None, "tp"), P("tp", None), P(None), P(None, None), P(None, None, "tp"), P(None, None, "tp"), P(None, "tp", None))
    out_specs = (P("dp", None), cache_spec, cache_spec)
    n_dp, n_tp = mesh.shape["dp"], mesh.shape["tp"]

    def layer_shard(hidden_in, k_cache, v_cache, seq_lens, chosen_experts, g_attn, w_q, w_k, w_v, w_o, g_moe, w_router, w_gate, w_up, w_down):
        rows, slots, heads, dim = k_cache.shape
        flat = (rows, slots * heads, dim)
        part, k_next, v_next = attention(
            hidden_in, k_cache.reshape(flat), v_cache.reshape(flat), seq_lens, g_attn, w_q, w_k, w_v, w_o)
        out = experts(part, hidden_in, chosen_experts.T, g_moe, w_router.T, w_gate.swapaxes(1, 2),
                      w_up.swapaxes(1, 2), w_down, n_dp, n_tp)
        return out, k_next.reshape(k_cache.shape), v_next.reshape(v_cache.shape)

    return jax.shard_map(layer_shard, mesh=mesh, in_specs=in_specs, out_specs=out_specs, check_vma=False)
```

```python
import functools
import math
import jax
import jax.numpy as jnp
from jax import lax
from jax.experimental import pallas as pl
from jax.experimental.pallas import tpu as pltpu
from jax.sharding import PartitionSpec as P

EPSILON = 1e-5
ROPE_THETA = 1000000.0
MASK_FILL = -1e30
MESH = pl.DeviceIdType.MESH
F32 = jnp.float32
BF16 = jnp.bfloat16
NT = (((1,), (1,)), ((), ()))
ANY = pl.BlockSpec(memory_space=pl.ANY)
VMEM = pl.BlockSpec(memory_space=pltpu.VMEM)
SMEM = pl.BlockSpec(memory_space=pltpu.SMEM)


def norm_rows(x32, gain):
    scale = lax.rsqrt(jnp.mean(x32 * x32, axis=-1, keepdims=True) + EPSILON)
    return (x32 * scale * gain).astype(BF16)


def gain_row(g_ref):
    g32 = g_ref[...].astype(F32)
    return jnp.concatenate([g32[i:i + 1, :] for i in range(g32.shape[0])], axis=1)


def attention_kernel(lens, x_hbm, g_ref, wq, wk, wv, wo, kc, vc, part_ref, kout, vout,
                     kbuf, vbuf, x_ref, qkvw, wobuf, qs, ks, vs, os_, wsem, insem, outsem, *, group):
    rows = x_ref.shape[0]
    width = wq.shape[1]
    heads = wq.shape[1] // 128
    slots = kc.shape[1]
    steps = rows // group
    half = steps // 2
    xcopy = pltpu.make_async_copy(x_hbm, x_ref, wsem.at[4])
    wcopies = [pltpu.make_async_copy(w, qkvw.at[:, pl.ds(i * width, width)], wsem.at[i])
               for i, w in enumerate((wq, wk, wv))]
    wocopy = pltpu.make_async_copy(wo, wobuf, wsem.at[3])
    xcopy.start()
    for cp in wcopies:
        cp.start()

    def fetch(i, hbm, buf, j):
        at = pl.ds(i * group, group)
        return pltpu.make_async_copy(hbm.at[at], buf.at[at], insem.at[j, i])

    def flush(i, hbm, buf, j):
        at = pl.ds(i * group, group)
        return pltpu.make_async_copy(buf.at[at], hbm.at[at], outsem.at[j, i])

    def fetch_groups(lo, hi):
        for i in range(lo, hi):
            fetch(i, kc, kbuf, 0).start()
            fetch(i, vc, vbuf, 1).start()

    row_id = lax.broadcasted_iota(jnp.int32, (rows, 128), 0)
    pos = jnp.zeros((rows, 128), jnp.int32)
    for b in range(rows):
        pos = jnp.where(row_id == b, lens[b], pos)
    lane = lax.broadcasted_iota(jnp.int32, (rows, 128), 1)
    freq = jnp.exp(lax.rem(lane, 64).astype(F32) * (-2.0 * math.log(ROPE_THETA) / 128))
    ang = pos.astype(F32) * freq
    cos_t = jnp.cos(ang)
    sin_t = jnp.sin(ang)
    sin_t = jnp.where(lane < 64, -sin_t, sin_t)

    def rope(u):
        return u * cos_t + pltpu.roll(u, 64, 1) * sin_t

    xcopy.wait()
    h = norm_rows(x_ref[...].astype(F32), gain_row(g_ref))
    fetch_groups(0, 1)
    for cp in wcopies:
        cp.wait()
    fetch_groups(1, half)
    qkv = jnp.dot(h, qkvw[...], preferred_element_type=F32)
    q, k, v = (qkv[:, i * width:(i + 1) * width] for i in range(3))
    fetch_groups(half, half + 2)
    for j in range(heads):
        cols = slice(128 * j, 128 * j + 128)
        qs[pl.ds(j, rows, stride=heads), :] = rope(q[:, cols]).astype(BF16).astype(F32)
        kj = rope(k[:, cols]).astype(BF16).astype(F32)
        vj = v[:, cols].astype(BF16).astype(F32)
        for rep in range(8 // heads):
            ks[pl.ds(j + rep * heads, rows, stride=8), :] = kj
            vs[pl.ds(j + rep * heads, rows, stride=8), :] = vj

    qrows = group * heads
    rid = lax.broadcasted_iota(jnp.int32, (qrows, slots), 0)
    cid = lax.broadcasted_iota(jnp.int32, (qrows, slots), 1)
    same_head = lax.rem(rid, heads) == lax.rem(cid, heads)
    slot = lax.div(cid, heads)
    seq_of = lax.div(rid, heads)
    oseq = lax.div(lax.broadcasted_iota(jnp.int32, (qrows, 128), 0), heads)
    trow = lax.div(lax.broadcasted_iota(jnp.int32, (16, 128), 0), heads)

    def insert(buf, new, b, p):
        at = pl.ds(pl.multiple_of(lax.div(p * heads, 16) * 16, 16), 16)
        n8 = new[pl.ds(pl.multiple_of(b * 8, 8), 8), :]
        n16 = jnp.concatenate([n8, n8], axis=0)
        old = buf[b, at, :].astype(F32)
        buf[b, at, :] = jnp.where(trow == lax.rem(p, 16 // heads), n16, old).astype(BF16)

    def step(i, carry):
        q16 = qs[pl.ds(pl.multiple_of(i * qrows, qrows), qrows), :].astype(BF16)
        fetch(i, kc, kbuf, 0).wait()
        ps = [lens[i * group + u] for u in range(group)]
        for u in range(group):
            insert(kbuf, ks, i * group + u, ps[u])
        @pl.when(i == 0)
        def _():
            fetch_groups(half + 2, steps)
            wocopy.start()

        @pl.when(i >= half)
        def _():
            flush(i, kout, kbuf, 0).start()

        sc = jnp.zeros((qrows, slots), F32)
        pm = jnp.zeros((qrows, slots), jnp.int32)
        for u in range(group):
            s_u = lax.dot_general(q16, kbuf[i * group + u], NT, preferred_element_type=F32)
            sc = jnp.where(seq_of == u, s_u, sc)
            pm = jnp.where(seq_of == u, ps[u], pm)
        sc = jnp.where(same_head & (slot <= pm), sc * (128 ** -0.5), MASK_FILL)
        ex = jnp.exp(sc - jnp.max(sc, axis=-1, keepdims=True))
        wt = (ex / jnp.sum(ex, axis=-1, keepdims=True)).astype(BF16)
        fetch(i, vc, vbuf, 1).wait()
        for u in range(group):
            insert(vbuf, vs, i * group + u, ps[u])

        @pl.when(i >= half)
        def _():
            flush(i, vout, vbuf, 1).start()

        @pl.when(i == half - 1)
        def _():
            for u in range(half):
                flush(u, kout, kbuf, 0).start()
                flush(u, vout, vbuf, 1).start()

        o = jnp.zeros((qrows, 128), F32)
        for u in range(group):
            o_u = jnp.dot(wt, vbuf[i * group + u], preferred_element_type=F32)
            o = jnp.where(oseq == u, o_u, o)
        os_[pl.ds(pl.multiple_of(i * qrows, qrows), qrows), :] = o
        return carry

    lax.fori_loop(0, steps, step, 0)
    o = jnp.concatenate([os_[pl.ds(j, rows, stride=heads), :] for j in range(heads)], axis=1).astype(BF16)
    wocopy.wait()
    part_ref[...] = jnp.dot(o, wobuf[...], preferred_element_type=F32)

    def drain(i, carry):
        flush(i, kout, kbuf, 0).wait()
        flush(i, vout, vbuf, 1).wait()
        return carry

    lax.fori_loop(0, steps, drain, 0)


def attention(x, kc, vc, lens, g, wq, wk, wv, wo):
    rows, d_model = x.shape
    _, slots, _ = kc.shape
    width = wq.shape[1]
    heads = width // 128
    group = 4
    steps = rows // group
    return pl.pallas_call(
        functools.partial(attention_kernel, group=group),
        name="attention",
        out_shape=(jax.ShapeDtypeStruct((rows, d_model), F32),
                   jax.ShapeDtypeStruct(kc.shape, BF16), jax.ShapeDtypeStruct(vc.shape, BF16)),
        in_specs=[SMEM, ANY, VMEM, ANY, ANY, ANY, ANY, ANY, ANY],
        out_specs=(VMEM, ANY, ANY),
        scratch_shapes=[
            pltpu.VMEM((rows, slots, 128), BF16),
            pltpu.VMEM((rows, slots, 128), BF16),
            pltpu.VMEM((rows, d_model), BF16),
            pltpu.VMEM((d_model, 3 * width), BF16),
            pltpu.VMEM((width, d_model), BF16),
            pltpu.VMEM((rows * heads, 128), F32),
            pltpu.VMEM((rows * 8, 128), F32),
            pltpu.VMEM((rows * 8, 128), F32),
            pltpu.VMEM((rows * heads, 128), F32),
            pltpu.SemaphoreType.DMA((5,)),
            pltpu.SemaphoreType.DMA((2, steps)),
            pltpu.SemaphoreType.DMA((2, steps)),
        ],
        compiler_params=pltpu.CompilerParams(vmem_limit_bytes=63 << 20),
        cost_estimate=pl.CostEstimate(flops=400_000_000, bytes_accessed=42_000_000, transcendentals=0),
    )(lens, x, g.reshape(-1, 128), wq, wk, wv, wo, kc, vc)


def experts_kernel(part_hbm, x_hbm, g_ref, picks, wr_hbm, wg, wu, wd, out_hbm,
                   part, x_ref, wr, lsem, osem, gbuf, ubuf, dbuf, xf, recv1, hall, hb, gall, z, acc, drecv, psum, frecv, yall,
                   gsem, usem, dsem, s1, r1, s2, r2, s3, r3, s4, r4, s5, r5, s6, r6, s7, r7, s8, r8,
                   *, n_dp, n_tp, n_exp, ring, batch, chunks):
    dp = lax.axis_index("dp")
    tp = lax.axis_index("tp")
    core = lax.rem(tp, 2)
    xx = lax.div(tp, 2)
    d_model = wg.shape[1]
    f_dim = wg.shape[0] // n_exp
    mine = n_exp // n_dp
    base = dp * mine
    batches = [(e, min(batch, mine - e)) for e in range(0, mine, batch)]
    n_chip = n_dp * n_tp // 2
    me_chip = dp * (n_tp // 2) + xx
    me = dp * n_tp + tp
    n_blk = n_dp * n_tp
    rows = x_ref.shape[0]
    cw = d_model // chunks

    def flip(v, bit):
        return 1 - v if bit else v

    def chip_peer(m):
        px = flip(xx, m & 1)
        pd = 2 * flip(lax.div(dp, 2), (m >> 2) & 1) + flip(lax.rem(dp, 2), (m >> 1) & 1)
        return pd, px

    peers = []
    for m in range(1, n_chip):
        pd, px = chip_peer(m)
        peers.append({"dp": pd, "tp": 2 * px + core})
    partner = {"dp": dp, "tp": 2 * xx + 1 - core}
    cross = {"dp": dp, "tp": 2 * (1 - xx) + 1 - core}

    def weights(b):
        e, n = batches[b]
        src = pl.ds(pl.multiple_of((base + e) * f_dim, f_dim), n * f_dim)
        s = b % ring
        return (pltpu.make_async_copy(wg.at[src], gbuf.at[s, pl.ds(0, n * f_dim)], gsem.at[s]),
                pltpu.make_async_copy(wu.at[src], ubuf.at[s, pl.ds(0, n * f_dim)], usem.at[s]))

    def down_weights(b):
        e, n = batches[b]
        src = pl.ds(pl.multiple_of((base + e) * f_dim, f_dim), n * f_dim)
        return pltpu.make_async_copy(wd.at[src], dbuf.at[pl.ds(e * f_dim, n * f_dim)], dsem.at[b])

    def start(b):
        for cp in weights(b):
            cp.start()

    barrier = pltpu.get_barrier_semaphore()
    for dev in peers + [partner, cross]:
        pl.semaphore_signal(barrier, inc=1, device_id=dev, device_id_type=MESH)
    loads = [pltpu.make_async_copy(a, b, lsem.at[i])
             for i, (a, b) in enumerate(((part_hbm, part), (x_hbm, x_ref), (wr_hbm, wr)))]
    for cp in loads:
        cp.start()
    start(0)
    for cp in loads:
        cp.wait()
    xf[...] = x_ref[...].astype(F32)
    pl.semaphore_wait(barrier, len(peers) + 2)

    def block(t):
        return pl.ds(pl.multiple_of(t * 8, 8), 8)

    first = []
    for k in range(1, n_tp):
        t_to = lax.rem(tp + k, n_tp)
        cp = pltpu.make_async_remote_copy(
            src_ref=part.at[block(t_to)], dst_ref=recv1.at[k - 1],
            send_sem=s1.at[k - 1], recv_sem=r1.at[k - 1],
            device_id={"dp": dp, "tp": t_to}, device_id_type=MESH)
        cp.start()
        first.append(cp)

    start(1)
    pick_cols = []
    row8 = lax.broadcasted_iota(jnp.int32, (8, 128), 0)
    for kk in range(picks.shape[0]):
        pc = jnp.zeros((8, 128), jnp.int32)
        for i in range(8):
            pc = jnp.where(row8 == i, picks[kk, tp * 8 + i], pc)
        pick_cols.append(pc)

    for cp in first:
        cp.wait()
    attn_sum = part[block(tp), :]
    for k in range(1, n_tp):
        attn_sum = attn_sum + recv1[k - 1]
    x1 = (xf[block(tp), :] + attn_sum).astype(BF16).astype(F32)
    xf[block(tp), :] = x1
    h2 = norm_rows(x1, gain_row(g_ref))
    hall[me] = h2

    def spread(buf, i, m, ssem, rsem):
        return pltpu.make_async_remote_copy(
            src_ref=buf.at[i], dst_ref=buf.at[i], send_sem=ssem.at[m], recv_sem=rsem.at[m],
            device_id=peers[m], device_id_type=MESH)

    def relay(buf, i, m, ssem, rsem):
        return pltpu.make_async_remote_copy(
            src_ref=buf.at[i], dst_ref=buf.at[i], send_sem=ssem.at[m], recv_sem=rsem.at[m],
            device_id=partner, device_id_type=MESH)

    order = sorted(range(n_chip - 1), key=lambda m: -bin(m + 1).count("1"))
    hs = [spread(hall, me, m, s2, r2) for m in range(n_chip - 1)]
    hd = [relay(hall, me, n_chip - 1, s3, r3)]
    for m in order:
        hs[m].start()
    hd[0].start()
    start(2)

    logits = lax.dot_general(h2, wr[...], NT, preferred_element_type=F32)
    lane = lax.broadcasted_iota(jnp.int32, (8, 128), 1)
    picked = []
    for pc in pick_cols:
        hit = (lane == pc)[:, :n_exp]
        picked.append(jnp.sum(jnp.where(hit, logits, 0.0), axis=1, keepdims=True))
    top = functools.reduce(jnp.maximum, picked)
    exs = [jnp.exp(p - top) for p in picked]
    den = functools.reduce(lambda a, b: a + b, exs)
    gates = jnp.zeros((8, 128), F32)
    for pc, ex in zip(pick_cols, exs):
        gates = gates + jnp.where(lane == pc, ex / den, 0.0)
    gall[me] = gates
    gs = [spread(gall, me, m, s4, r4) for m in range(n_chip - 1)]
    gd = [relay(gall, me, n_chip - 1, s5, r5)]
    for m in order:
        gs[m].start()
    gd[0].start()

    def owner(m):
        pd, px = chip_peer(m + 1)
        return pd * n_tp + 2 * px + core

    for m in reversed(order):
        hs[m].wait_recv()
        cp = relay(hall, owner(m), m, s3, r3)
        cp.start()
        hd.append(cp)
    for m in reversed(order):
        gs[m].wait_recv()
        cp = relay(gall, owner(m), m, s5, r5)
        cp.start()
        gd.append(cp)
    for cp in hd + gd:
        cp.wait_recv()
    for cp in hs + gs + hd + gd:
        cp.wait_send()

    for r in range(n_blk // 2):
        two = jnp.concatenate([hall[2 * r].astype(F32), hall[2 * r + 1].astype(F32)], axis=0)
        hb[16 * r:16 * r + 16, :] = two.astype(BF16)
    gmat = gall[...].reshape(n_blk * 8, 128)
    glane = lax.broadcasted_iota(jnp.int32, (n_blk * 8, 128), 1)

    def products(b):
        s, width = b % ring, batches[b][1] * f_dim
        for cp in weights(b):
            cp.wait()
        gate = lax.dot_general(hb[...], gbuf[s, :width], NT, preferred_element_type=F32)
        up = lax.dot_general(hb[...], ubuf[s, :width], NT, preferred_element_type=F32)
        if b + ring < len(batches):
            start(b + ring)
        return gate, up

    def activate(b, gate, up):
        e0, n = batches[b]
        cols = [jnp.sum(jnp.where(glane == base + e, gmat, 0.0), axis=1, keepdims=True)
                for e in range(e0, e0 + n)]
        for lo in range(0, n * f_dim, 128):
            hi = min(lo + 128, n * f_dim)
            ea, eb = lo // f_dim, (hi - 1) // f_dim
            gcol = cols[ea]
            if eb > ea:
                gcol = jnp.where(glane[:, :hi - lo] < eb * f_dim - lo, cols[ea], cols[eb])
            ga = gate[:, lo:hi]
            at = e0 * f_dim + lo
            z[:, at:at + hi - lo] = (gcol * (ga * jax.nn.sigmoid(ga)) * up[:, lo:hi]).astype(BF16)

    for b in range(len(batches)):
        down_weights(b).start()
    before = None
    for b in range(len(batches)):
        now = products(b)
        if before is not None:
            activate(b - 1, *before)
        before = now
    activate(len(batches) - 1, *before)
    for b in range(len(batches)):
        down_weights(b).wait()

    lag = 1
    finals = {}
    pair = {}

    def pair_sum(n):
        pair[n].wait_recv()
        psum[n] = acc[n, core] + drecv[n]
        for m in order:
            pd, px = chip_peer(m + 1)
            chip = pd * (n_tp // 2) + px
            cp = pltpu.make_async_remote_copy(
                src_ref=psum.at[n, block(chip)], dst_ref=frecv.at[n, m],
                send_sem=s7.at[n, m], recv_sem=r7.at[n, m], device_id=peers[m], device_id_type=MESH)
            cp.start()
            finals[n, m] = cp

    for n in range(chunks):
        res = jnp.dot(z[...], dbuf[:, n * cw:(n + 1) * cw], preferred_element_type=F32)
        for j in range(n_chip):
            for q in range(2):
                at = (2 * j + q) * 8
                acc[n, q, 8 * j:8 * j + 8, :] = res[at:at + 8, :]
        cp = pltpu.make_async_remote_copy(
            src_ref=acc.at[n, 1 - core], dst_ref=drecv.at[n], send_sem=s6.at[n], recv_sem=r6.at[n],
            device_id=partner, device_id_type=MESH)
        cp.start()
        pair[n] = cp
        if n >= lag:
            pair_sum(n - lag)
    for n in range(chunks - lag, chunks):
        pair_sum(n)
    last = []
    for n in range(chunks):
        total = psum[n, block(me_chip), :]
        for m in range(n_chip - 1):
            finals[n, m].wait_recv()
            total = total + frecv[n, m]
        cols = slice(n * cw, (n + 1) * cw)
        yall[tp, :, cols] = (xf[block(tp), cols] + total).astype(BF16)
        if n % 2 == 1:
            span = pl.ds((n - 1) * cw, 2 * cw)
            for k in range(1, n_tp):
                t_to = lax.rem(tp + k, n_tp)
                cp = pltpu.make_async_remote_copy(
                    src_ref=yall.at[tp, :, span], dst_ref=yall.at[tp, :, span],
                    send_sem=s8.at[n // 2, k - 1], recv_sem=r8.at[n // 2, k - 1],
                    device_id={"dp": dp, "tp": t_to}, device_id_type=MESH)
                cp.start()
                last.append(cp)
    outs = []
    for n in range(chunks // 2):
        span = pl.ds(2 * n * cw, 2 * cw)
        for cp in last[n * (n_tp - 1):(n + 1) * (n_tp - 1)]:
            cp.wait_recv()
        cp = pltpu.make_async_copy(yall.at[:, :, span], out_hbm.at[:, :, span], osem.at[n])
        cp.start()
        outs.append(cp)
    for cp in outs:
        cp.wait()
    for cp in last + list(pair.values()) + list(finals.values()):
        cp.wait_send()


def experts(part, x, picks, g, wr, wg, wu, wd, n_dp, n_tp):
    rows, d_model = x.shape
    n_exp, f_dim, _ = wg.shape
    mine = n_exp // n_dp
    ring, batch, chunks = 3, 4, 4
    n_batch = -(-mine // batch)
    wg, wu, wd = (w.reshape(n_exp * f_dim, d_model) for w in (wg, wu, wd))
    n_chip = n_dp * n_tp // 2
    cw = d_model // chunks
    dma = pltpu.SemaphoreType.DMA
    out = pl.pallas_call(
        functools.partial(experts_kernel, n_dp=n_dp, n_tp=n_tp, n_exp=n_exp, ring=ring, batch=batch,
                          chunks=chunks),
        name="experts",
        out_shape=jax.ShapeDtypeStruct((n_tp, 8, d_model), BF16),
        in_specs=[ANY, ANY, VMEM, SMEM, ANY, ANY, ANY, ANY],
        out_specs=ANY,
        scratch_shapes=[
            pltpu.VMEM((rows, d_model), F32),
            pltpu.VMEM((rows, d_model), BF16),
            pltpu.VMEM(wr.shape, BF16),
            dma((3,)), dma((chunks // 2,)),
            pltpu.VMEM((ring, batch * f_dim, d_model), BF16),
            pltpu.VMEM((ring, batch * f_dim, d_model), BF16),
            pltpu.VMEM((mine * f_dim, d_model), BF16),
            pltpu.VMEM((rows, d_model), F32),
            pltpu.VMEM((n_tp - 1, 8, d_model), F32),
            pltpu.VMEM((n_dp * n_tp, 8, d_model), BF16),
            pltpu.VMEM((n_dp * n_tp * 8, d_model), BF16),
            pltpu.VMEM((n_dp * n_tp, 8, 128), F32),
            pltpu.VMEM((n_dp * n_tp * 8, mine * f_dim), BF16),
            pltpu.VMEM((chunks, 2, n_chip * 8, cw), F32),
            pltpu.VMEM((chunks, n_chip * 8, cw), F32),
            pltpu.VMEM((chunks, n_chip * 8, cw), F32),
            pltpu.VMEM((chunks, n_chip - 1, 8, cw), F32),
            pltpu.VMEM((n_tp, 8, d_model), BF16),
            dma((ring,)), dma((ring,)), dma((n_batch,)),
            dma((n_tp - 1,)), dma((n_tp - 1,)),
            dma((n_chip - 1,)), dma((n_chip - 1,)),
            dma((n_chip,)), dma((n_chip,)),
            dma((n_chip - 1,)), dma((n_chip - 1,)),
            dma((n_chip,)), dma((n_chip,)),
            dma((chunks,)), dma((chunks,)),
            dma((chunks, n_chip - 1)), dma((chunks, n_chip - 1)),
            dma((chunks // 2, n_tp - 1)), dma((chunks // 2, n_tp - 1)),
        ],
        compiler_params=pltpu.CompilerParams(
            collective_id=0, has_side_effects=True, vmem_limit_bytes=63 << 20),
        cost_estimate=pl.CostEstimate(flops=8_000_000_000, bytes_accessed=66_000_000, transcendentals=0),
    )(part, x, g.reshape(-1, 128), picks, wr, wg, wu, wd)
    return out.reshape(rows, d_model)


def solution(mesh):
    cache_spec = P("dp", None, "tp", None)
    in_specs = (P("dp", None), cache_spec, cache_spec, P("dp"), P("dp", None), P(None), P(None, "tp"), P(None, "tp"), P(None, "tp"), P("tp", None), P(None), P(None, None), P(None, None, "tp"), P(None, None, "tp"), P(None, "tp", None))
    out_specs = (P("dp", None), cache_spec, cache_spec)
    n_dp, n_tp = mesh.shape["dp"], mesh.shape["tp"]

    def layer_shard(hidden_in, k_cache, v_cache, seq_lens, chosen_experts, g_attn, w_q, w_k, w_v, w_o, g_moe, w_router, w_gate, w_up, w_down):
        rows, slots, heads, dim = k_cache.shape
        flat = (rows, slots * heads, dim)
        part, k_next, v_next = attention(
            hidden_in, k_cache.reshape(flat), v_cache.reshape(flat), seq_lens, g_attn, w_q, w_k, w_v, w_o)
        out = experts(part, hidden_in, chosen_experts.T, g_moe, w_router.T, w_gate.swapaxes(1, 2),
                      w_up.swapaxes(1, 2), w_down, n_dp, n_tp)
        return out, k_next.reshape(k_cache.shape), v_next.reshape(v_cache.shape)

    return jax.shard_map(layer_shard, mesh=mesh, in_specs=in_specs, out_specs=out_specs, check_vma=False)
```

```python
import functools
import math
import jax
import jax.numpy as jnp
from jax import lax
from jax.experimental import pallas as pl
from jax.experimental.pallas import tpu as pltpu
from jax.sharding import PartitionSpec as P

EPSILON = 1e-5
ROPE_THETA = 1000000.0
MASK_FILL = -1e30
MESH = pl.DeviceIdType.MESH
F32 = jnp.float32
BF16 = jnp.bfloat16
NT = (((1,), (1,)), ((), ()))
ANY = pl.BlockSpec(memory_space=pl.ANY)
VMEM = pl.BlockSpec(memory_space=pltpu.VMEM)
SMEM = pl.BlockSpec(memory_space=pltpu.SMEM)


def norm_rows(x32, gain):
    scale = lax.rsqrt(jnp.mean(x32 * x32, axis=-1, keepdims=True) + EPSILON)
    return (x32 * scale * gain).astype(BF16)


def gain_row(g_ref):
    g32 = g_ref[...].astype(F32)
    return jnp.concatenate([g32[i:i + 1, :] for i in range(g32.shape[0])], axis=1)


def attention_kernel(lens, x_hbm, g_ref, wq, wk, wv, wo, kc, vc, part_ref, kout, vout,
                     kbuf, vbuf, x_ref, qkvw, wobuf, qs, ks, vs, os_, wsem, insem, outsem, *, group):
    rows = x_ref.shape[0]
    width = wq.shape[1]
    heads = wq.shape[1] // 128
    slots = kc.shape[1]
    steps = rows // group
    half = steps // 2
    xcopy = pltpu.make_async_copy(x_hbm, x_ref, wsem.at[4])
    wcopies = [pltpu.make_async_copy(w, qkvw.at[:, pl.ds(i * width, width)], wsem.at[i])
               for i, w in enumerate((wq, wk, wv))]
    wocopy = pltpu.make_async_copy(wo, wobuf, wsem.at[3])
    xcopy.start()
    for cp in wcopies:
        cp.start()

    def fetch(i, hbm, buf, j):
        at = pl.ds(i * group, group)
        return pltpu.make_async_copy(hbm.at[at], buf.at[at], insem.at[j, i])

    def flush(i, hbm, buf, j):
        at = pl.ds(i * group, group)
        return pltpu.make_async_copy(buf.at[at], hbm.at[at], outsem.at[j, i])

    def fetch_groups(lo, hi):
        for i in range(lo, hi):
            fetch(i, kc, kbuf, 0).start()
            fetch(i, vc, vbuf, 1).start()

    row_id = lax.broadcasted_iota(jnp.int32, (rows, 128), 0)
    pos = jnp.zeros((rows, 128), jnp.int32)
    for b in range(rows):
        pos = jnp.where(row_id == b, lens[b], pos)
    lane = lax.broadcasted_iota(jnp.int32, (rows, 128), 1)
    freq = jnp.exp(lax.rem(lane, 64).astype(F32) * (-2.0 * math.log(ROPE_THETA) / 128))
    ang = pos.astype(F32) * freq
    cos_t = jnp.cos(ang)
    sin_t = jnp.sin(ang)
    sin_t = jnp.where(lane < 64, -sin_t, sin_t)

    def rope(u):
        return u * cos_t + pltpu.roll(u, 64, 1) * sin_t

    xcopy.wait()
    h = norm_rows(x_ref[...].astype(F32), gain_row(g_ref))
    fetch_groups(0, 1)
    for cp in wcopies:
        cp.wait()
    fetch_groups(1, half)
    qkv = jnp.dot(h, qkvw[...], preferred_element_type=F32)
    q, k, v = (qkv[:, i * width:(i + 1) * width] for i in range(3))
    fetch_groups(half, half + 2)
    for j in range(heads):
        cols = slice(128 * j, 128 * j + 128)
        qs[pl.ds(j, rows, stride=heads), :] = rope(q[:, cols]).astype(BF16).astype(F32)
        kj = rope(k[:, cols]).astype(BF16).astype(F32)
        vj = v[:, cols].astype(BF16).astype(F32)
        for rep in range(8 // heads):
            ks[pl.ds(j + rep * heads, rows, stride=8), :] = kj
            vs[pl.ds(j + rep * heads, rows, stride=8), :] = vj

    qrows = group * heads
    rid = lax.broadcasted_iota(jnp.int32, (qrows, slots), 0)
    cid = lax.broadcasted_iota(jnp.int32, (qrows, slots), 1)
    same_head = lax.rem(rid, heads) == lax.rem(cid, heads)
    slot = lax.div(cid, heads)
    seq_of = lax.div(rid, heads)
    oseq = lax.div(lax.broadcasted_iota(jnp.int32, (qrows, 128), 0), heads)
    trow = lax.div(lax.broadcasted_iota(jnp.int32, (16, 128), 0), heads)

    def insert(buf, new, b, p):
        at = pl.ds(pl.multiple_of(lax.div(p * heads, 16) * 16, 16), 16)
        n8 = new[pl.ds(pl.multiple_of(b * 8, 8), 8), :]
        n16 = jnp.concatenate([n8, n8], axis=0)
        old = buf[b, at, :].astype(F32)
        buf[b, at, :] = jnp.where(trow == lax.rem(p, 16 // heads), n16, old).astype(BF16)

    def step(i, carry):
        q16 = qs[pl.ds(pl.multiple_of(i * qrows, qrows), qrows), :].astype(BF16)
        fetch(i, kc, kbuf, 0).wait()
        ps = [lens[i * group + u] for u in range(group)]
        for u in range(group):
            insert(kbuf, ks, i * group + u, ps[u])
        @pl.when(i == 0)
        def _():
            fetch_groups(half + 2, steps)
            wocopy.start()

        @pl.when(i >= half)
        def _():
            flush(i, kout, kbuf, 0).start()

        sc = jnp.zeros((qrows, slots), F32)
        pm = jnp.zeros((qrows, slots), jnp.int32)
        for u in range(group):
            s_u = lax.dot_general(q16, kbuf[i * group + u], NT, preferred_element_type=F32)
            sc = jnp.where(seq_of == u, s_u, sc)
            pm = jnp.where(seq_of == u, ps[u], pm)
        sc = jnp.where(same_head & (slot <= pm), sc * (128 ** -0.5), MASK_FILL)
        ex = jnp.exp(sc - jnp.max(sc, axis=-1, keepdims=True))
        wt = (ex / jnp.sum(ex, axis=-1, keepdims=True)).astype(BF16)
        fetch(i, vc, vbuf, 1).wait()
        for u in range(group):
            insert(vbuf, vs, i * group + u, ps[u])

        @pl.when(i >= half)
        def _():
            flush(i, vout, vbuf, 1).start()

        @pl.when(i == half - 1)
        def _():
            for u in range(half):
                flush(u, kout, kbuf, 0).start()
                flush(u, vout, vbuf, 1).start()

        o = jnp.zeros((qrows, 128), F32)
        for u in range(group):
            o_u = jnp.dot(wt, vbuf[i * group + u], preferred_element_type=F32)
            o = jnp.where(oseq == u, o_u, o)
        os_[pl.ds(pl.multiple_of(i * qrows, qrows), qrows), :] = o
        return carry

    lax.fori_loop(0, steps, step, 0)
    o = jnp.concatenate([os_[pl.ds(j, rows, stride=heads), :] for j in range(heads)], axis=1).astype(BF16)
    wocopy.wait()
    part_ref[...] = jnp.dot(o, wobuf[...], preferred_element_type=F32)

    def drain(i, carry):
        flush(i, kout, kbuf, 0).wait()
        flush(i, vout, vbuf, 1).wait()
        return carry

    lax.fori_loop(0, steps, drain, 0)


def attention(x, kc, vc, lens, g, wq, wk, wv, wo):
    rows, d_model = x.shape
    _, slots, _ = kc.shape
    width = wq.shape[1]
    heads = width // 128
    group = 4
    steps = rows // group
    return pl.pallas_call(
        functools.partial(attention_kernel, group=group),
        name="attention",
        out_shape=(jax.ShapeDtypeStruct((rows, d_model), F32),
                   jax.ShapeDtypeStruct(kc.shape, BF16), jax.ShapeDtypeStruct(vc.shape, BF16)),
        in_specs=[SMEM, ANY, VMEM, ANY, ANY, ANY, ANY, ANY, ANY],
        out_specs=(VMEM, ANY, ANY),
        scratch_shapes=[
            pltpu.VMEM((rows, slots, 128), BF16),
            pltpu.VMEM((rows, slots, 128), BF16),
            pltpu.VMEM((rows, d_model), BF16),
            pltpu.VMEM((d_model, 3 * width), BF16),
            pltpu.VMEM((width, d_model), BF16),
            pltpu.VMEM((rows * heads, 128), F32),
            pltpu.VMEM((rows * 8, 128), F32),
            pltpu.VMEM((rows * 8, 128), F32),
            pltpu.VMEM((rows * heads, 128), F32),
            pltpu.SemaphoreType.DMA((5,)),
            pltpu.SemaphoreType.DMA((2, steps)),
            pltpu.SemaphoreType.DMA((2, steps)),
        ],
        compiler_params=pltpu.CompilerParams(vmem_limit_bytes=63 << 20),
        cost_estimate=pl.CostEstimate(flops=400_000_000, bytes_accessed=42_000_000, transcendentals=0),
    )(lens, x, g.reshape(-1, 128), wq, wk, wv, wo, kc, vc)


def experts_kernel(part_hbm, x_hbm, g_ref, picks, wr_hbm, wg, wu, wd, out_hbm,
                   part, x_ref, wr, lsem, osem, gbuf, ubuf, dbuf, xf, recv1, hall, hb, gall, gt, z, acc, drecv, psum, frecv, yall,
                   gsem, usem, dsem, s1, r1, s2, r2, s3, r3, s4, r4, s5, r5, s6, r6, s7, r7, s8, r8,
                   *, n_dp, n_tp, n_exp, ring, batch, chunks):
    dp = lax.axis_index("dp")
    tp = lax.axis_index("tp")
    core = lax.rem(tp, 2)
    xx = lax.div(tp, 2)
    d_model = wg.shape[1]
    f_dim = wg.shape[0] // n_exp
    mine = n_exp // n_dp
    base = dp * mine
    batches = [(e, min(batch, mine - e)) for e in range(0, mine, batch)]
    n_chip = n_dp * n_tp // 2
    me_chip = dp * (n_tp // 2) + xx
    me = dp * n_tp + tp
    n_blk = n_dp * n_tp
    rows = x_ref.shape[0]
    cw = d_model // chunks

    def flip(v, bit):
        return 1 - v if bit else v

    def chip_peer(m):
        px = flip(xx, m & 1)
        pd = 2 * flip(lax.div(dp, 2), (m >> 2) & 1) + flip(lax.rem(dp, 2), (m >> 1) & 1)
        return pd, px

    peers = []
    for m in range(1, n_chip):
        pd, px = chip_peer(m)
        peers.append({"dp": pd, "tp": 2 * px + core})
    partner = {"dp": dp, "tp": 2 * xx + 1 - core}
    cross = {"dp": dp, "tp": 2 * (1 - xx) + 1 - core}

    def weights(b):
        e, n = batches[b]
        src = pl.ds(pl.multiple_of((base + e) * f_dim, f_dim), n * f_dim)
        s = b % ring
        return (pltpu.make_async_copy(wg.at[src], gbuf.at[s, pl.ds(0, n * f_dim)], gsem.at[s]),
                pltpu.make_async_copy(wu.at[src], ubuf.at[s, pl.ds(0, n * f_dim)], usem.at[s]))

    def down_weights(b):
        e, n = batches[b]
        src = pl.ds(pl.multiple_of((base + e) * f_dim, f_dim), n * f_dim)
        return pltpu.make_async_copy(wd.at[src], dbuf.at[pl.ds(e * f_dim, n * f_dim)], dsem.at[b])

    def start(b):
        for cp in weights(b):
            cp.start()

    barrier = pltpu.get_barrier_semaphore()
    for dev in peers + [partner, cross]:
        pl.semaphore_signal(barrier, inc=1, device_id=dev, device_id_type=MESH)
    loads = [pltpu.make_async_copy(a, b, lsem.at[i])
             for i, (a, b) in enumerate(((part_hbm, part), (x_hbm, x_ref), (wr_hbm, wr)))]
    for cp in loads:
        cp.start()
    for cp in loads:
        cp.wait()
    start(0)
    xf[...] = x_ref[...].astype(F32)
    pl.semaphore_wait(barrier, len(peers) + 2)

    def block(t):
        return pl.ds(pl.multiple_of(t * 8, 8), 8)

    first = []
    for k in range(1, n_tp):
        t_to = lax.rem(tp + k, n_tp)
        cp = pltpu.make_async_remote_copy(
            src_ref=part.at[block(t_to)], dst_ref=recv1.at[k - 1],
            send_sem=s1.at[k - 1], recv_sem=r1.at[k - 1],
            device_id={"dp": dp, "tp": t_to}, device_id_type=MESH)
        cp.start()
        first.append(cp)

    start(1)
    pick_cols = []
    row8 = lax.broadcasted_iota(jnp.int32, (8, 128), 0)
    for kk in range(picks.shape[0]):
        pc = jnp.zeros((8, 128), jnp.int32)
        for i in range(8):
            pc = jnp.where(row8 == i, picks[kk, tp * 8 + i], pc)
        pick_cols.append(pc)

    for cp in first:
        cp.wait()
    attn_sum = part[block(tp), :]
    for k in range(1, n_tp):
        attn_sum = attn_sum + recv1[k - 1]
    x1 = (xf[block(tp), :] + attn_sum).astype(BF16).astype(F32)
    xf[block(tp), :] = x1
    h2 = norm_rows(x1, gain_row(g_ref))
    hall[me] = h2

    def spread(buf, i, m, ssem, rsem):
        return pltpu.make_async_remote_copy(
            src_ref=buf.at[i], dst_ref=buf.at[i], send_sem=ssem.at[m], recv_sem=rsem.at[m],
            device_id=peers[m], device_id_type=MESH)

    def relay(buf, i, m, ssem, rsem):
        return pltpu.make_async_remote_copy(
            src_ref=buf.at[i], dst_ref=buf.at[i], send_sem=ssem.at[m], recv_sem=rsem.at[m],
            device_id=partner, device_id_type=MESH)

    order = sorted(range(n_chip - 1), key=lambda m: -bin(m + 1).count("1"))
    hs = [spread(hall, me, m, s2, r2) for m in range(n_chip - 1)]
    hd = [relay(hall, me, n_chip - 1, s3, r3)]
    for m in order:
        hs[m].start()
    hd[0].start()
    start(2)

    logits = lax.dot_general(h2, wr[...], NT, preferred_element_type=F32)
    lane = lax.broadcasted_iota(jnp.int32, (8, 128), 1)
    picked = []
    for pc in pick_cols:
        hit = (lane == pc)[:, :n_exp]
        picked.append(jnp.sum(jnp.where(hit, logits, 0.0), axis=1, keepdims=True))
    top = functools.reduce(jnp.maximum, picked)
    exs = [jnp.exp(p - top) for p in picked]
    den = functools.reduce(lambda a, b: a + b, exs)
    gates = jnp.zeros((8, 128), F32)
    for pc, ex in zip(pick_cols, exs):
        gates = gates + jnp.where(lane == pc, ex / den, 0.0)
    gall[me] = gates
    gs = [spread(gall, me, m, s4, r4) for m in range(n_chip - 1)]
    gd = [relay(gall, me, n_chip - 1, s5, r5)]
    for m in order:
        gs[m].start()
    gd[0].start()

    def owner(m):
        pd, px = chip_peer(m + 1)
        return pd * n_tp + 2 * px + core

    for m in reversed(order):
        hs[m].wait_recv()
        cp = relay(hall, owner(m), m, s3, r3)
        cp.start()
        hd.append(cp)
    for cp in hd:
        cp.wait_recv()

    for r in range(n_blk // 2):
        two = jnp.concatenate([hall[2 * r].astype(F32), hall[2 * r + 1].astype(F32)], axis=0)
        hb[16 * r:16 * r + 16, :] = two.astype(BF16)
    def products(b):
        s, width = b % ring, batches[b][1] * f_dim
        for cp in weights(b):
            cp.wait()
        gate = lax.dot_general(gbuf[s, :width], hb[...], NT, preferred_element_type=F32)
        up = lax.dot_general(ubuf[s, :width], hb[...], NT, preferred_element_type=F32)
        if b + ring < len(batches):
            start(b + ring)
        return gate, up

    def activate(b, gate, up):
        e0, n = batches[b]
        brow = lax.broadcasted_iota(jnp.int32, (128, n_blk * 8), 0)
        rows_g = [gt[pl.ds(base + e, 1), :] for e in range(e0, e0 + n)]
        for lo in range(0, n * f_dim, 128):
            hi = min(lo + 128, n * f_dim)
            ea, eb = lo // f_dim, (hi - 1) // f_dim
            grow = rows_g[ea]
            if eb > ea:
                grow = jnp.where(brow[:hi - lo] < eb * f_dim - lo, rows_g[ea], rows_g[eb])
            ga = gate[lo:hi]
            at = e0 * f_dim + lo
            zt = (grow * (ga * jax.nn.sigmoid(ga)) * up[lo:hi]).astype(BF16)
            z[:, at:at + hi - lo] = zt.T

    for b in range(len(batches)):
        down_weights(b).start()
    before = None
    for b in range(len(batches)):
        now = products(b)
        if b == 0:
            for m in reversed(order):
                gs[m].wait_recv()
                cp = relay(gall, owner(m), m, s5, r5)
                cp.start()
                gd.append(cp)
        if b == 1:
            for cp in gd:
                cp.wait_recv()
            gt[...] = gall[...].reshape(n_blk * 8, 128).T
        if before is not None:
            activate(b - 1, *before)
        before = now
    activate(len(batches) - 1, *before)
    for b in range(len(batches)):
        down_weights(b).wait()

    lag = 1
    finals = {}
    pair = {}

    def pair_sum(n):
        pair[n].wait_recv()
        psum[n] = acc[n, core] + drecv[n]
        for m in order:
            pd, px = chip_peer(m + 1)
            chip = pd * (n_tp // 2) + px
            cp = pltpu.make_async_remote_copy(
                src_ref=psum.at[n, block(chip)], dst_ref=frecv.at[n, m],
                send_sem=s7.at[n, m], recv_sem=r7.at[n, m], device_id=peers[m], device_id_type=MESH)
            cp.start()
            finals[n, m] = cp

    for n in range(chunks):
        res = jnp.dot(z[...], dbuf[:, n * cw:(n + 1) * cw], preferred_element_type=F32)
        for j in range(n_chip):
            for q in range(2):
                at = (2 * j + q) * 8
                acc[n, q, 8 * j:8 * j + 8, :] = res[at:at + 8, :]
        cp = pltpu.make_async_remote_copy(
            src_ref=acc.at[n, 1 - core], dst_ref=drecv.at[n], send_sem=s6.at[n], recv_sem=r6.at[n],
            device_id=partner, device_id_type=MESH)
        cp.start()
        pair[n] = cp
        if n >= lag:
            pair_sum(n - lag)
    for n in range(chunks - lag, chunks):
        pair_sum(n)
    last = []
    for n in range(chunks):
        total = psum[n, block(me_chip), :]
        for m in range(n_chip - 1):
            finals[n, m].wait_recv()
            total = total + frecv[n, m]
        cols = slice(n * cw, (n + 1) * cw)
        yall[tp, :, cols] = (xf[block(tp), cols] + total).astype(BF16)
        span = pl.ds(n * cw, cw)
        for k in (2, 1, 3):
            t_to = lax.rem(tp + k, n_tp)
            cp = pltpu.make_async_remote_copy(
                src_ref=yall.at[tp, :, span], dst_ref=yall.at[tp, :, span],
                send_sem=s8.at[n, k - 1], recv_sem=r8.at[n, k - 1],
                device_id={"dp": dp, "tp": t_to}, device_id_type=MESH)
            cp.start()
            last.append(cp)
    outs = []
    for n in range(chunks):
        span = pl.ds(n * cw, cw)
        for cp in last[n * (n_tp - 1):(n + 1) * (n_tp - 1)]:
            cp.wait_recv()
        cp = pltpu.make_async_copy(yall.at[:, :, span], out_hbm.at[:, :, span], osem.at[n])
        cp.start()
        outs.append(cp)
    for cp in hs + gs + hd + gd + list(pair.values()) + list(finals.values()) + last:
        cp.wait_send()
    for cp in outs:
        cp.wait()


def experts(part, x, picks, g, wr, wg, wu, wd, n_dp, n_tp):
    rows, d_model = x.shape
    n_exp, f_dim, _ = wg.shape
    mine = n_exp // n_dp
    ring, batch, chunks = 3, 4, 4
    n_batch = -(-mine // batch)
    wg, wu, wd = (w.reshape(n_exp * f_dim, d_model) for w in (wg, wu, wd))
    n_chip = n_dp * n_tp // 2
    cw = d_model // chunks
    dma = pltpu.SemaphoreType.DMA
    out = pl.pallas_call(
        functools.partial(experts_kernel, n_dp=n_dp, n_tp=n_tp, n_exp=n_exp, ring=ring, batch=batch,
                          chunks=chunks),
        name="experts",
        out_shape=jax.ShapeDtypeStruct((n_tp, 8, d_model), BF16),
        in_specs=[ANY, ANY, VMEM, SMEM, ANY, ANY, ANY, ANY],
        out_specs=ANY,
        scratch_shapes=[
            pltpu.VMEM((rows, d_model), F32),
            pltpu.VMEM((rows, d_model), BF16),
            pltpu.VMEM(wr.shape, BF16),
            dma((3,)), dma((chunks,)),
            pltpu.VMEM((ring, batch * f_dim, d_model), BF16),
            pltpu.VMEM((ring, batch * f_dim, d_model), BF16),
            pltpu.VMEM((mine * f_dim, d_model), BF16),
            pltpu.VMEM((rows, d_model), F32),
            pltpu.VMEM((n_tp - 1, 8, d_model), F32),
            pltpu.VMEM((n_dp * n_tp, 8, d_model), BF16),
            pltpu.VMEM((n_dp * n_tp * 8, d_model), BF16),
            pltpu.VMEM((n_dp * n_tp, 8, 128), F32),
            pltpu.VMEM((128, n_dp * n_tp * 8), F32),
            pltpu.VMEM((n_dp * n_tp * 8, mine * f_dim), BF16),
            pltpu.VMEM((chunks, 2, n_chip * 8, cw), F32),
            pltpu.VMEM((chunks, n_chip * 8, cw), F32),
            pltpu.VMEM((chunks, n_chip * 8, cw), F32),
            pltpu.VMEM((chunks, n_chip - 1, 8, cw), F32),
            pltpu.VMEM((n_tp, 8, d_model), BF16),
            dma((ring,)), dma((ring,)), dma((n_batch,)),
            dma((n_tp - 1,)), dma((n_tp - 1,)),
            dma((n_chip - 1,)), dma((n_chip - 1,)),
            dma((n_chip,)), dma((n_chip,)),
            dma((n_chip - 1,)), dma((n_chip - 1,)),
            dma((n_chip,)), dma((n_chip,)),
            dma((chunks,)), dma((chunks,)),
            dma((chunks, n_chip - 1)), dma((chunks, n_chip - 1)),
            dma((chunks, n_tp - 1)), dma((chunks, n_tp - 1)),
        ],
        compiler_params=pltpu.CompilerParams(
            collective_id=0, has_side_effects=True, vmem_limit_bytes=63 << 20),
        cost_estimate=pl.CostEstimate(flops=8_000_000_000, bytes_accessed=66_000_000, transcendentals=0),
    )(part, x, g.reshape(-1, 128), picks, wr, wg, wu, wd)
    return out.reshape(rows, d_model)


def solution(mesh):
    cache_spec = P("dp", None, "tp", None)
    in_specs = (P("dp", None), cache_spec, cache_spec, P("dp"), P("dp", None), P(None), P(None, "tp"), P(None, "tp"), P(None, "tp"), P("tp", None), P(None), P(None, None), P(None, None, "tp"), P(None, None, "tp"), P(None, "tp", None))
    out_specs = (P("dp", None), cache_spec, cache_spec)
    n_dp, n_tp = mesh.shape["dp"], mesh.shape["tp"]

    def layer_shard(hidden_in, k_cache, v_cache, seq_lens, chosen_experts, g_attn, w_q, w_k, w_v, w_o, g_moe, w_router, w_gate, w_up, w_down):
        rows, slots, heads, dim = k_cache.shape
        flat = (rows, slots * heads, dim)
        part, k_next, v_next = attention(
            hidden_in, k_cache.reshape(flat), v_cache.reshape(flat), seq_lens, g_attn, w_q, w_k, w_v, w_o)
        out = experts(part, hidden_in, chosen_experts.T, g_moe, w_router.T, w_gate.swapaxes(1, 2),
                      w_up.swapaxes(1, 2), w_down, n_dp, n_tp)
        return out, k_next.reshape(k_cache.shape), v_next.reshape(v_cache.shape)

    return jax.shard_map(layer_shard, mesh=mesh, in_specs=in_specs, out_specs=out_specs, check_vma=False)
```

```python
import functools
import math
import jax
import jax.numpy as jnp
from jax import lax
from jax.experimental import pallas as pl
from jax.experimental.pallas import tpu as pltpu
from jax.sharding import PartitionSpec as P

EPSILON = 1e-5
ROPE_THETA = 1000000.0
MASK_FILL = -1e30
MESH = pl.DeviceIdType.MESH
F32 = jnp.float32
BF16 = jnp.bfloat16
NT = (((1,), (1,)), ((), ()))
ANY = pl.BlockSpec(memory_space=pl.ANY)
VMEM = pl.BlockSpec(memory_space=pltpu.VMEM)


def norm_rows(x32, gain):
    scale = lax.rsqrt(jnp.mean(x32 * x32, axis=-1, keepdims=True) + EPSILON)
    return (x32 * scale * gain).astype(BF16)


def gain_row(g_ref):
    g32 = g_ref[...].astype(F32)
    return jnp.concatenate([g32[i:i + 1, :] for i in range(g32.shape[0])], axis=1)


def attention_kernel(lens_hbm, x_hbm, g_hbm, wq, wk, wv, wo, kc, vc, part_ref, kout, vout,
                     kbuf, vbuf, lens, x_ref, g_ref, qkvw, wobuf, qs, ks, vs, os_, wsem, insem, outsem, *, group):
    rows = x_ref.shape[0]
    width = wq.shape[1]
    heads = wq.shape[1] // 128
    slots = kc.shape[1]
    steps = rows // group
    half = steps // 2
    small = [pltpu.make_async_copy(a, b, wsem.at[4 + i])
             for i, (a, b) in enumerate(((lens_hbm, lens), (x_hbm, x_ref), (g_hbm, g_ref)))]
    wcopies = [pltpu.make_async_copy(w, qkvw.at[:, pl.ds(i * width, width)], wsem.at[i])
               for i, w in enumerate((wq, wk, wv))]
    wocopy = pltpu.make_async_copy(wo, wobuf, wsem.at[3])
    for cp in small + wcopies:
        cp.start()

    def fetch(i, hbm, buf, j):
        at = pl.ds(i * group, group)
        return pltpu.make_async_copy(hbm.at[at], buf.at[at], insem.at[j, i])

    def flush(i, hbm, buf, j):
        at = pl.ds(i * group, group)
        return pltpu.make_async_copy(buf.at[at], hbm.at[at], outsem.at[j])

    def fetch_groups(lo, hi):
        for i in range(lo, hi):
            fetch(i, kc, kbuf, 0).start()
            fetch(i, vc, vbuf, 1).start()

    small[0].wait()
    row_id = lax.broadcasted_iota(jnp.int32, (rows, 128), 0)
    pos = jnp.zeros((rows, 128), jnp.int32)
    for b in range(rows):
        pos = jnp.where(row_id == b, lens[b], pos)
    lane = lax.broadcasted_iota(jnp.int32, (rows, 128), 1)
    freq = jnp.exp(lax.rem(lane, 64).astype(F32) * (-2.0 * math.log(ROPE_THETA) / 128))
    ang = pos.astype(F32) * freq
    cos_t = jnp.cos(ang)
    sin_t = jnp.sin(ang)
    sin_t = jnp.where(lane < 64, -sin_t, sin_t)

    def rope(u):
        return u * cos_t + pltpu.roll(u, 64, 1) * sin_t

    for cp in small[1:]:
        cp.wait()
    h = norm_rows(x_ref[...].astype(F32), gain_row(g_ref))
    fetch_groups(0, 1)
    for cp in wcopies:
        cp.wait()
    fetch_groups(1, half)
    qkv = jnp.dot(h, qkvw[...], preferred_element_type=F32)
    q, k, v = (qkv[:, i * width:(i + 1) * width] for i in range(3))
    fetch_groups(half, half + 2)
    for j in range(heads):
        cols = slice(128 * j, 128 * j + 128)
        qs[pl.ds(j, rows, stride=heads), :] = rope(q[:, cols]).astype(BF16).astype(F32)
        kj = rope(k[:, cols]).astype(BF16).astype(F32)
        vj = v[:, cols].astype(BF16).astype(F32)
        for rep in range(8 // heads):
            ks[pl.ds(j + rep * heads, rows, stride=8), :] = kj
            vs[pl.ds(j + rep * heads, rows, stride=8), :] = vj

    qrows = group * heads
    rid = lax.broadcasted_iota(jnp.int32, (qrows, slots), 0)
    cid = lax.broadcasted_iota(jnp.int32, (qrows, slots), 1)
    same_head = lax.rem(rid, heads) == lax.rem(cid, heads)
    slot = lax.div(cid, heads)
    seq_of = lax.div(rid, heads)
    oseq = lax.div(lax.broadcasted_iota(jnp.int32, (qrows, 128), 0), heads)
    trow = lax.div(lax.broadcasted_iota(jnp.int32, (16, 128), 0), heads)

    def insert(buf, new, b, p):
        at = pl.ds(pl.multiple_of(lax.div(p * heads, 16) * 16, 16), 16)
        n8 = new[pl.ds(pl.multiple_of(b * 8, 8), 8), :]
        n16 = jnp.concatenate([n8, n8], axis=0)
        old = buf[b, at, :].astype(F32)
        buf[b, at, :] = jnp.where(trow == lax.rem(p, 16 // heads), n16, old).astype(BF16)

    def step(i, carry):
        q16 = qs[pl.ds(pl.multiple_of(i * qrows, qrows), qrows), :].astype(BF16)
        fetch(i, kc, kbuf, 0).wait()
        ps = [lens[i * group + u] for u in range(group)]
        for u in range(group):
            insert(kbuf, ks, i * group + u, ps[u])
        @pl.when(i == 0)
        def _():
            fetch_groups(half + 2, steps)
            wocopy.start()

        @pl.when(i >= half)
        def _():
            flush(i, kout, kbuf, 0).start()

        sc = jnp.zeros((qrows, slots), F32)
        pm = jnp.zeros((qrows, slots), jnp.int32)
        for u in range(group):
            s_u = lax.dot_general(q16, kbuf[i * group + u], NT, preferred_element_type=F32)
            sc = jnp.where(seq_of == u, s_u, sc)
            pm = jnp.where(seq_of == u, ps[u], pm)
        sc = jnp.where(same_head & (slot <= pm), sc * (128 ** -0.5), MASK_FILL)
        ex = jnp.exp(sc - jnp.max(sc, axis=-1, keepdims=True))
        wt = (ex / jnp.sum(ex, axis=-1, keepdims=True)).astype(BF16)
        fetch(i, vc, vbuf, 1).wait()
        for u in range(group):
            insert(vbuf, vs, i * group + u, ps[u])

        @pl.when(i >= half)
        def _():
            flush(i, vout, vbuf, 1).start()

        @pl.when(i == half - 1)
        def _():
            for u in range(half):
                flush(u, kout, kbuf, 0).start()
                flush(u, vout, vbuf, 1).start()

        o = jnp.zeros((qrows, 128), F32)
        for u in range(group):
            o_u = jnp.dot(wt, vbuf[i * group + u], preferred_element_type=F32)
            o = jnp.where(oseq == u, o_u, o)
        os_[pl.ds(pl.multiple_of(i * qrows, qrows), qrows), :] = o
        return carry

    lax.fori_loop(0, steps, step, 0)
    o = jnp.concatenate([os_[pl.ds(j, rows, stride=heads), :] for j in range(heads)], axis=1).astype(BF16)
    wocopy.wait()
    part_ref[...] = jnp.dot(o, wobuf[...], preferred_element_type=F32)

    pltpu.make_async_copy(kbuf, kout, outsem.at[0]).wait()
    pltpu.make_async_copy(vbuf, vout, outsem.at[1]).wait()


def attention(x, kc, vc, lens, g, wq, wk, wv, wo):
    rows, d_model = x.shape
    _, slots, _ = kc.shape
    width = wq.shape[1]
    heads = width // 128
    group = 4
    steps = rows // group
    return pl.pallas_call(
        functools.partial(attention_kernel, group=group),
        name="attention",
        out_shape=(jax.ShapeDtypeStruct((rows, d_model), F32),
                   jax.ShapeDtypeStruct(kc.shape, BF16), jax.ShapeDtypeStruct(vc.shape, BF16)),
        in_specs=[ANY] * 9,
        out_specs=(VMEM, ANY, ANY),
        scratch_shapes=[
            pltpu.VMEM((rows, slots, 128), BF16),
            pltpu.VMEM((rows, slots, 128), BF16),
            pltpu.SMEM(lens.shape, jnp.int32),
            pltpu.VMEM((rows, d_model), BF16),
            pltpu.VMEM((d_model // 128, 128), BF16),
            pltpu.VMEM((d_model, 3 * width), BF16),
            pltpu.VMEM((width, d_model), BF16),
            pltpu.VMEM((rows * heads, 128), F32),
            pltpu.VMEM((rows * 8, 128), F32),
            pltpu.VMEM((rows * 8, 128), F32),
            pltpu.VMEM((rows * heads, 128), F32),
            pltpu.SemaphoreType.DMA((7,)),
            pltpu.SemaphoreType.DMA((2, steps)),
            pltpu.SemaphoreType.DMA((2,)),
        ],
        compiler_params=pltpu.CompilerParams(vmem_limit_bytes=63 << 20),
        cost_estimate=pl.CostEstimate(flops=400_000_000, bytes_accessed=42_000_000, transcendentals=0),
    )(lens, x, g.reshape(-1, 128), wq, wk, wv, wo, kc, vc)


def experts_kernel(part_hbm, x_hbm, g_hbm, picks_hbm, wr_hbm, wg, wu, wd, out_hbm,
                   part, x_ref, g_ref, picks, wr, lsem, osem, gbuf, ubuf, dbuf, xf, recv1, hall, hb, gall, gt, z, acc, drecv, psum, frecv, yall,
                   gsem, usem, dsem, s1, r1, s2, r2, s3, r3, s4, r4, s5, r5, s6, r6, s7, r7, s8, r8,
                   *, n_dp, n_tp, n_exp, ring, batch, chunks):
    dp = lax.axis_index("dp")
    tp = lax.axis_index("tp")
    core = lax.rem(tp, 2)
    xx = lax.div(tp, 2)
    d_model = wg.shape[1]
    f_dim = wg.shape[0] // n_exp
    mine = n_exp // n_dp
    base = dp * mine
    batches = [(e, min(batch, mine - e)) for e in range(0, mine, batch)]
    n_chip = n_dp * n_tp // 2
    me_chip = dp * (n_tp // 2) + xx
    me = dp * n_tp + tp
    n_blk = n_dp * n_tp
    rows = x_ref.shape[0]
    cw = d_model // chunks

    def flip(v, bit):
        return 1 - v if bit else v

    def chip_peer(m):
        px = flip(xx, m & 1)
        pd = 2 * flip(lax.div(dp, 2), (m >> 2) & 1) + flip(lax.rem(dp, 2), (m >> 1) & 1)
        return pd, px

    peers = []
    for m in range(1, n_chip):
        pd, px = chip_peer(m)
        peers.append({"dp": pd, "tp": 2 * px + core})
    partner = {"dp": dp, "tp": 2 * xx + 1 - core}
    cross = {"dp": dp, "tp": 2 * (1 - xx) + 1 - core}

    def weights(b):
        e, n = batches[b]
        src = pl.ds(pl.multiple_of((base + e) * f_dim, f_dim), n * f_dim)
        s = b % ring
        return (pltpu.make_async_copy(wg.at[src], gbuf.at[s, pl.ds(0, n * f_dim)], gsem.at[s]),
                pltpu.make_async_copy(wu.at[src], ubuf.at[s, pl.ds(0, n * f_dim)], usem.at[s]))

    def down_weights(b):
        e, n = batches[b]
        src = pl.ds(pl.multiple_of((base + e) * f_dim, f_dim), n * f_dim)
        return pltpu.make_async_copy(wd.at[src], dbuf.at[pl.ds(e * f_dim, n * f_dim)], dsem.at[b])

    def start(b):
        for cp in weights(b):
            cp.start()

    barrier = pltpu.get_barrier_semaphore()
    for dev in peers + [partner, cross]:
        pl.semaphore_signal(barrier, inc=1, device_id=dev, device_id_type=MESH)
    loads = [pltpu.make_async_copy(a, b, lsem.at[i])
             for i, (a, b) in enumerate(((part_hbm, part), (x_hbm, x_ref), (g_hbm, g_ref),
                                     (picks_hbm, picks), (wr_hbm, wr)))]
    for cp in loads:
        cp.start()
    loads[0].wait()
    pl.semaphore_wait(barrier, len(peers) + 2)

    def block(t):
        return pl.ds(pl.multiple_of(t * 8, 8), 8)

    first = []
    for k in range(1, n_tp):
        t_to = lax.rem(tp + k, n_tp)
        cp = pltpu.make_async_remote_copy(
            src_ref=part.at[block(t_to)], dst_ref=recv1.at[k - 1],
            send_sem=s1.at[k - 1], recv_sem=r1.at[k - 1],
            device_id={"dp": dp, "tp": t_to}, device_id_type=MESH)
        cp.start()
        first.append(cp)

    for cp in loads[1:]:
        cp.wait()
    start(0)
    start(1)
    xf[...] = x_ref[...].astype(F32)
    pick_cols = []
    row8 = lax.broadcasted_iota(jnp.int32, (8, 128), 0)
    for kk in range(picks.shape[0]):
        pc = jnp.zeros((8, 128), jnp.int32)
        for i in range(8):
            pc = jnp.where(row8 == i, picks[kk, tp * 8 + i], pc)
        pick_cols.append(pc)

    for cp in first:
        cp.wait()
    attn_sum = part[block(tp), :]
    for k in range(1, n_tp):
        attn_sum = attn_sum + recv1[k - 1]
    x1 = (xf[block(tp), :] + attn_sum).astype(BF16).astype(F32)
    xf[block(tp), :] = x1
    h2 = norm_rows(x1, gain_row(g_ref))
    hall[me] = h2

    def wait_all(ref, sem):
        pltpu.make_async_copy(ref, ref, sem).wait()

    def spread(buf, i, m, ssem, rsem):
        return pltpu.make_async_remote_copy(
            src_ref=buf.at[i], dst_ref=buf.at[i], send_sem=ssem, recv_sem=rsem,
            device_id=peers[m], device_id_type=MESH)

    def relay(buf, i, m, ssem, rsem):
        return pltpu.make_async_remote_copy(
            src_ref=buf.at[i], dst_ref=buf.at[i], send_sem=ssem, recv_sem=rsem,
            device_id=partner, device_id_type=MESH)

    order = sorted(range(n_chip - 1), key=lambda m: -bin(m + 1).count("1"))
    hs = [spread(hall, me, m, s2.at[0], r2.at[m]) for m in range(n_chip - 1)]
    hd = [relay(hall, me, n_chip - 1, s3.at[0], r3.at[0])]
    for m in order:
        hs[m].start()
    hd[0].start()
    start(2)

    logits = lax.dot_general(h2, wr[...], NT, preferred_element_type=F32)
    lane = lax.broadcasted_iota(jnp.int32, (8, 128), 1)
    picked = []
    for pc in pick_cols:
        hit = (lane == pc)[:, :n_exp]
        picked.append(jnp.sum(jnp.where(hit, logits, 0.0), axis=1, keepdims=True))
    top = functools.reduce(jnp.maximum, picked)
    exs = [jnp.exp(p - top) for p in picked]
    den = functools.reduce(lambda a, b: a + b, exs)
    gates = jnp.zeros((8, 128), F32)
    for pc, ex in zip(pick_cols, exs):
        gates = gates + jnp.where(lane == pc, ex / den, 0.0)
    gall[me] = gates
    gs = [spread(gall, me, m, s4.at[0], r4.at[0]) for m in range(n_chip - 1)]
    gd = [relay(gall, me, n_chip - 1, s5.at[0], r5.at[0])]
    for m in order:
        gs[m].start()
    gd[0].start()

    def owner(m):
        pd, px = chip_peer(m + 1)
        return pd * n_tp + 2 * px + core

    for m in reversed(order):
        hs[m].wait_recv()
        cp = relay(hall, owner(m), m, s3.at[0], r3.at[0])
        cp.start()
        hd.append(cp)
    wait_all(hall.at[pl.ds(0, n_chip)], r3.at[0])

    for r in range(n_blk // 2):
        two = jnp.concatenate([hall[2 * r].astype(F32), hall[2 * r + 1].astype(F32)], axis=0)
        hb[16 * r:16 * r + 16, :] = two.astype(BF16)
    def products(b):
        s, width = b % ring, batches[b][1] * f_dim
        for cp in weights(b):
            cp.wait()
        gate = lax.dot_general(gbuf[s, :width], hb[...], NT, preferred_element_type=F32)
        up = lax.dot_general(ubuf[s, :width], hb[...], NT, preferred_element_type=F32)
        if b + ring < len(batches):
            start(b + ring)
        return gate, up

    def activate(b, gate, up):
        e0, n = batches[b]
        brow = lax.broadcasted_iota(jnp.int32, (128, n_blk * 8), 0)
        rows_g = [gt[pl.ds(base + e, 1), :] for e in range(e0, e0 + n)]
        for lo in range(0, n * f_dim, 128):
            hi = min(lo + 128, n * f_dim)
            ea, eb = lo // f_dim, (hi - 1) // f_dim
            grow = rows_g[ea]
            if eb > ea:
                grow = jnp.where(brow[:hi - lo] < eb * f_dim - lo, rows_g[ea], rows_g[eb])
            ga = gate[lo:hi]
            at = e0 * f_dim + lo
            zt = (grow * (ga * jax.nn.sigmoid(ga)) * up[lo:hi]).astype(BF16)
            z[:, at:at + hi - lo] = zt.T

    for b in range(len(batches)):
        down_weights(b).start()
    before = None
    for b in range(len(batches)):
        now = products(b)
        if b == 0:
            wait_all(gall.at[pl.ds(0, n_chip - 1)], r4.at[0])
            for m in order:
                cp = relay(gall, owner(m), m, s5.at[0], r5.at[0])
                cp.start()
                gd.append(cp)
        if b == 1:
            wait_all(gall.at[pl.ds(0, n_chip)], r5.at[0])
            gt[...] = gall[...].reshape(n_blk * 8, 128).T
        if before is not None:
            activate(b - 1, *before)
        before = now
    activate(len(batches) - 1, *before)
    for b in range(len(batches)):
        down_weights(b).wait()

    lag = 1
    finals = {}
    pair = {}

    def pair_sum(n):
        pair[n].wait_recv()
        psum[n] = acc[n, core] + drecv[n]
        for m in order:
            pd, px = chip_peer(m + 1)
            chip = pd * (n_tp // 2) + px
            cp = pltpu.make_async_remote_copy(
                src_ref=psum.at[n, block(chip)], dst_ref=frecv.at[n, m],
                send_sem=s7.at[0], recv_sem=r7.at[n], device_id=peers[m], device_id_type=MESH)
            cp.start()
            finals[n, m] = cp

    for n in range(chunks):
        cols = slice(n * cw, (n + 1) * cw)
        res = jnp.dot(z[...], dbuf[:, cols], preferred_element_type=F32)
        for j in range(n_chip):
            for q in range(2):
                at = (2 * j + q) * 8
                acc[n, q, 8 * j:8 * j + 8, :] = res[at:at + 8, :]
        cp = pltpu.make_async_remote_copy(
            src_ref=acc.at[n, 1 - core], dst_ref=drecv.at[n], send_sem=s6.at[0], recv_sem=r6.at[n],
            device_id=partner, device_id_type=MESH)
        cp.start()
        pair[n] = cp
        if n >= lag:
            pair_sum(n - lag)
    for n in range(chunks - lag, chunks):
        pair_sum(n)
    last, outs = [], []
    for n in range(chunks):
        total = psum[n, block(me_chip), :]
        wait_all(frecv.at[n], r7.at[n])
        for m in range(n_chip - 1):
            total = total + frecv[n, m]
        cols = slice(n * cw, (n + 1) * cw)
        yall[:, cols] = (xf[block(tp), cols] + total).astype(BF16)
        if n % 2 == 0:
            continue
        span = pl.ds((n - 1) * cw, 2 * cw)
        cp = pltpu.make_async_copy(yall.at[:, span], out_hbm.at[tp, :, span], osem.at[n // 2])
        cp.start()
        outs.append(cp)
        for k in (2, 1, 3):
            t_to = lax.rem(tp + k, n_tp)
            cp = pltpu.make_async_remote_copy(
                src_ref=yall.at[:, span], dst_ref=out_hbm.at[tp, :, span],
                send_sem=s8.at[0], recv_sem=r8.at[0],
                device_id={"dp": dp, "tp": t_to}, device_id_type=MESH)
            cp.start()
            last.append(cp)
    wait_all(out_hbm.at[pl.ds(0, n_tp - 1)], r8.at[0])
    wait_all(hall.at[pl.ds(0, n_chip - 1)], s2.at[0])
    wait_all(hall.at[pl.ds(0, n_chip)], s3.at[0])
    wait_all(gall.at[pl.ds(0, n_chip - 1)], s4.at[0])
    wait_all(gall.at[pl.ds(0, n_chip)], s5.at[0])
    wait_all(drecv, s6.at[0])
    wait_all(frecv, s7.at[0])
    wait_all(hall.at[pl.ds(0, n_tp - 1)], s8.at[0])
    for cp in outs:
        cp.wait()


def experts(part, x, picks, g, wr, wg, wu, wd, n_dp, n_tp):
    rows, d_model = x.shape
    n_exp, f_dim, _ = wg.shape
    mine = n_exp // n_dp
    ring, batch, chunks = 3, 4, 4
    n_batch = -(-mine // batch)
    wg, wu, wd = (w.reshape(n_exp * f_dim, d_model) for w in (wg, wu, wd))
    n_chip = n_dp * n_tp // 2
    cw = d_model // chunks
    dma = pltpu.SemaphoreType.DMA
    out = pl.pallas_call(
        functools.partial(experts_kernel, n_dp=n_dp, n_tp=n_tp, n_exp=n_exp, ring=ring, batch=batch,
                          chunks=chunks),
        name="experts",
        out_shape=jax.ShapeDtypeStruct((n_tp, 8, d_model), BF16),
        in_specs=[ANY] * 8,
        out_specs=ANY,
        scratch_shapes=[
            pltpu.VMEM((rows, d_model), F32),
            pltpu.VMEM((rows, d_model), BF16),
            pltpu.VMEM((d_model // 128, 128), BF16),
            pltpu.SMEM(picks.shape, jnp.int32),
            pltpu.VMEM(wr.shape, BF16),
            dma((5,)), dma((chunks // 2,)),
            pltpu.VMEM((ring, batch * f_dim, d_model), BF16),
            pltpu.VMEM((ring, batch * f_dim, d_model), BF16),
            pltpu.VMEM((mine * f_dim, d_model), BF16),
            pltpu.VMEM((rows, d_model), F32),
            pltpu.VMEM((n_tp - 1, 8, d_model), F32),
            pltpu.VMEM((n_dp * n_tp, 8, d_model), BF16),
            pltpu.VMEM((n_dp * n_tp * 8, d_model), BF16),
            pltpu.VMEM((n_dp * n_tp, 8, 128), F32),
            pltpu.VMEM((128, n_dp * n_tp * 8), F32),
            pltpu.VMEM((n_dp * n_tp * 8, mine * f_dim), BF16),
            pltpu.VMEM((chunks, 2, n_chip * 8, cw), F32),
            pltpu.VMEM((chunks, n_chip * 8, cw), F32),
            pltpu.VMEM((chunks, n_chip * 8, cw), F32),
            pltpu.VMEM((chunks, n_chip - 1, 8, cw), F32),
            pltpu.VMEM((8, d_model), BF16),
            dma((ring,)), dma((ring,)), dma((n_batch,)),
            dma((n_tp - 1,)), dma((n_tp - 1,)),
            dma((1,)), dma((n_chip - 1,)),
            dma((1,)), dma((1,)),
            dma((1,)), dma((1,)),
            dma((1,)), dma((1,)),
            dma((1,)), dma((chunks,)),
            dma((1,)), dma((chunks,)),
            dma((1,)), dma((1,)),
        ],
        compiler_params=pltpu.CompilerParams(
            collective_id=0, has_side_effects=True, vmem_limit_bytes=63 << 20),
        cost_estimate=pl.CostEstimate(flops=8_000_000_000, bytes_accessed=66_000_000, transcendentals=0),
    )(part, x, g.reshape(-1, 128), picks, wr, wg, wu, wd)
    return out.reshape(rows, d_model)


def solution(mesh):
    cache_spec = P("dp", None, "tp", None)
    in_specs = (P("dp", None), cache_spec, cache_spec, P("dp"), P("dp", None), P(None), P(None, "tp"), P(None, "tp"), P(None, "tp"), P("tp", None), P(None), P(None, None), P(None, None, "tp"), P(None, None, "tp"), P(None, "tp", None))
    out_specs = (P("dp", None), cache_spec, cache_spec)
    n_dp, n_tp = mesh.shape["dp"], mesh.shape["tp"]

    def layer_shard(hidden_in, k_cache, v_cache, seq_lens, chosen_experts, g_attn, w_q, w_k, w_v, w_o, g_moe, w_router, w_gate, w_up, w_down):
        rows, slots, heads, dim = k_cache.shape
        flat = (rows, slots * heads, dim)
        part, k_next, v_next = attention(
            hidden_in, k_cache.reshape(flat), v_cache.reshape(flat), seq_lens, g_attn, w_q, w_k, w_v, w_o)
        out = experts(part, hidden_in, chosen_experts.T, g_moe, w_router.T, w_gate.swapaxes(1, 2),
                      w_up.swapaxes(1, 2), w_down, n_dp, n_tp)
        return out, k_next.reshape(k_cache.shape), v_next.reshape(v_cache.shape)

    return jax.shard_map(layer_shard, mesh=mesh, in_specs=in_specs, out_specs=out_specs, check_vma=False)
```

```python
import functools
import math
import jax
import jax.numpy as jnp
from jax import lax
from jax.experimental import pallas as pl
from jax.experimental.pallas import tpu as pltpu
from jax.sharding import PartitionSpec as P

EPSILON = 1e-5
ROPE_THETA = 1000000.0
MASK_FILL = -1e30
MESH = pl.DeviceIdType.MESH
F32 = jnp.float32
BF16 = jnp.bfloat16
NT = (((1,), (1,)), ((), ()))
ANY = pl.BlockSpec(memory_space=pl.ANY)
VMEM = pl.BlockSpec(memory_space=pltpu.VMEM)


def norm_rows(x32, gain):
    scale = lax.rsqrt(jnp.mean(x32 * x32, axis=-1, keepdims=True) + EPSILON)
    return (x32 * scale * gain).astype(BF16)


def gain_row(g_ref):
    g32 = g_ref[...].astype(F32)
    return jnp.concatenate([g32[i:i + 1, :] for i in range(g32.shape[0])], axis=1)


def attention_kernel(lens_hbm, x_hbm, g_hbm, wq, wk, wv, wo, kc, vc, part_ref, kout, vout,
                     kbuf, vbuf, lens, x_ref, g_ref, qkvw, wobuf, qs, ks, vs, os_, wsem, insem, outsem, *, group):
    rows = x_ref.shape[0]
    width = wq.shape[1]
    heads = wq.shape[1] // 128
    slots = kc.shape[1]
    steps = rows // group
    half = steps // 2
    small = [pltpu.make_async_copy(a, b, wsem.at[4 + i])
             for i, (a, b) in enumerate(((lens_hbm, lens), (x_hbm, x_ref), (g_hbm, g_ref)))]
    wcopies = [pltpu.make_async_copy(w, qkvw.at[:, pl.ds(i * width, width)], wsem.at[i])
               for i, w in enumerate((wq, wk, wv))]
    wocopy = pltpu.make_async_copy(wo, wobuf, wsem.at[3])
    for cp in small + wcopies:
        cp.start()

    def fetch(i, hbm, buf, j):
        at = pl.ds(i * group, group)
        return pltpu.make_async_copy(hbm.at[at], buf.at[at], insem.at[j, i])

    def flush(i, hbm, buf, j):
        at = pl.ds(i * group, group)
        return pltpu.make_async_copy(buf.at[at], hbm.at[at], outsem.at[j])

    def fetch_groups(lo, hi):
        for i in range(lo, hi):
            fetch(i, kc, kbuf, 0).start()
            fetch(i, vc, vbuf, 1).start()

    small[0].wait()
    row_id = lax.broadcasted_iota(jnp.int32, (rows, 128), 0)
    pos = jnp.zeros((rows, 128), jnp.int32)
    for b in range(rows):
        pos = jnp.where(row_id == b, lens[b], pos)
    lane = lax.broadcasted_iota(jnp.int32, (rows, 128), 1)
    freq = jnp.exp(lax.rem(lane, 64).astype(F32) * (-2.0 * math.log(ROPE_THETA) / 128))
    ang = pos.astype(F32) * freq
    cos_t = jnp.cos(ang)
    sin_t = jnp.sin(ang)
    sin_t = jnp.where(lane < 64, -sin_t, sin_t)

    def rope(u):
        return u * cos_t + pltpu.roll(u, 64, 1) * sin_t

    for cp in small[1:]:
        cp.wait()
    h = norm_rows(x_ref[...].astype(F32), gain_row(g_ref))
    fetch_groups(0, 1)
    for cp in wcopies:
        cp.wait()
    fetch_groups(1, half)
    qkv = jnp.dot(h, qkvw[...], preferred_element_type=F32)
    q, k, v = (qkv[:, i * width:(i + 1) * width] for i in range(3))
    fetch_groups(half, half + 2)
    for j in range(heads):
        cols = slice(128 * j, 128 * j + 128)
        qs[pl.ds(j, rows, stride=heads), :] = rope(q[:, cols]).astype(BF16).astype(F32)
        kj = rope(k[:, cols]).astype(BF16).astype(F32)
        vj = v[:, cols].astype(BF16).astype(F32)
        for rep in range(8 // heads):
            ks[pl.ds(j + rep * heads, rows, stride=8), :] = kj
            vs[pl.ds(j + rep * heads, rows, stride=8), :] = vj

    qrows = group * heads
    rid = lax.broadcasted_iota(jnp.int32, (qrows, slots), 0)
    cid = lax.broadcasted_iota(jnp.int32, (qrows, slots), 1)
    same_head = lax.rem(rid, heads) == lax.rem(cid, heads)
    slot = lax.div(cid, heads)
    seq_of = lax.div(rid, heads)
    oseq = lax.div(lax.broadcasted_iota(jnp.int32, (qrows, 128), 0), heads)
    trow = lax.div(lax.broadcasted_iota(jnp.int32, (16, 128), 0), heads)

    def insert(buf, new, b, p):
        at = pl.ds(pl.multiple_of(lax.div(p * heads, 16) * 16, 16), 16)
        n8 = new[pl.ds(pl.multiple_of(b * 8, 8), 8), :]
        n16 = jnp.concatenate([n8, n8], axis=0)
        old = buf[b, at, :].astype(F32)
        buf[b, at, :] = jnp.where(trow == lax.rem(p, 16 // heads), n16, old).astype(BF16)

    def step(i, carry):
        q16 = qs[pl.ds(pl.multiple_of(i * qrows, qrows), qrows), :].astype(BF16)
        fetch(i, kc, kbuf, 0).wait()
        ps = [lens[i * group + u] for u in range(group)]
        for u in range(group):
            insert(kbuf, ks, i * group + u, ps[u])
        @pl.when(i == 0)
        def _():
            fetch_groups(half + 2, steps)
            wocopy.start()

        @pl.when(i >= half)
        def _():
            flush(i, kout, kbuf, 0).start()

        sc = jnp.zeros((qrows, slots), F32)
        pm = jnp.zeros((qrows, slots), jnp.int32)
        for u in range(group):
            s_u = lax.dot_general(q16, kbuf[i * group + u], NT, preferred_element_type=F32)
            sc = jnp.where(seq_of == u, s_u, sc)
            pm = jnp.where(seq_of == u, ps[u], pm)
        sc = jnp.where(same_head & (slot <= pm), sc * (128 ** -0.5), MASK_FILL)
        ex = jnp.exp(sc - jnp.max(sc, axis=-1, keepdims=True))
        wt = (ex / jnp.sum(ex, axis=-1, keepdims=True)).astype(BF16)
        fetch(i, vc, vbuf, 1).wait()
        for u in range(group):
            insert(vbuf, vs, i * group + u, ps[u])

        @pl.when(i >= half)
        def _():
            flush(i, vout, vbuf, 1).start()

        @pl.when(i == half - 1)
        def _():
            for u in range(half):
                flush(u, kout, kbuf, 0).start()
                flush(u, vout, vbuf, 1).start()

        o = jnp.zeros((qrows, 128), F32)
        for u in range(group):
            o_u = jnp.dot(wt, vbuf[i * group + u], preferred_element_type=F32)
            o = jnp.where(oseq == u, o_u, o)
        os_[pl.ds(pl.multiple_of(i * qrows, qrows), qrows), :] = o
        return carry

    lax.fori_loop(0, steps, step, 0)
    o = jnp.concatenate([os_[pl.ds(j, rows, stride=heads), :] for j in range(heads)], axis=1).astype(BF16)
    wocopy.wait()
    part_ref[...] = jnp.dot(o, wobuf[...], preferred_element_type=F32)

    pltpu.make_async_copy(kbuf, kout, outsem.at[0]).wait()
    pltpu.make_async_copy(vbuf, vout, outsem.at[1]).wait()


def attention(x, kc, vc, lens, g, wq, wk, wv, wo):
    rows, d_model = x.shape
    _, slots, _ = kc.shape
    width = wq.shape[1]
    heads = width // 128
    group = 4
    steps = rows // group
    return pl.pallas_call(
        functools.partial(attention_kernel, group=group),
        name="attention",
        out_shape=(jax.ShapeDtypeStruct((rows, d_model), F32),
                   jax.ShapeDtypeStruct(kc.shape, BF16), jax.ShapeDtypeStruct(vc.shape, BF16)),
        in_specs=[ANY] * 9,
        out_specs=(VMEM, ANY, ANY),
        scratch_shapes=[
            pltpu.VMEM((rows, slots, 128), BF16),
            pltpu.VMEM((rows, slots, 128), BF16),
            pltpu.SMEM(lens.shape, jnp.int32),
            pltpu.VMEM((rows, d_model), BF16),
            pltpu.VMEM((d_model // 128, 128), BF16),
            pltpu.VMEM((d_model, 3 * width), BF16),
            pltpu.VMEM((width, d_model), BF16),
            pltpu.VMEM((rows * heads, 128), F32),
            pltpu.VMEM((rows * 8, 128), F32),
            pltpu.VMEM((rows * 8, 128), F32),
            pltpu.VMEM((rows * heads, 128), F32),
            pltpu.SemaphoreType.DMA((7,)),
            pltpu.SemaphoreType.DMA((2, steps)),
            pltpu.SemaphoreType.DMA((2,)),
        ],
        compiler_params=pltpu.CompilerParams(vmem_limit_bytes=63 << 20),
        cost_estimate=pl.CostEstimate(flops=400_000_000, bytes_accessed=42_000_000, transcendentals=0),
    )(lens, x, g.reshape(-1, 128), wq, wk, wv, wo, kc, vc)


def experts_kernel(part_hbm, x_hbm, g_hbm, picks_hbm, wr_hbm, wg, wu, wd, out_hbm,
                   part, x_ref, g_ref, picks, wr, lsem, osem, gbuf, ubuf, dbuf, xf, recv1, hall, hb, gall, gt, z, acc, drecv, psum, frecv, yall,
                   gsem, usem, dsem, s1, r1, s2, r2, s3, r3, s4, r4, s5, r5, s6, r6, s7, r7, s8, r8,
                   *, n_dp, n_tp, n_exp, ring, batch, chunks):
    dp = lax.axis_index("dp")
    tp = lax.axis_index("tp")
    core = lax.rem(tp, 2)
    xx = lax.div(tp, 2)
    d_model = wg.shape[1]
    f_dim = wg.shape[0] // n_exp
    mine = n_exp // n_dp
    base = dp * mine
    batches = [(e, min(batch, mine - e)) for e in range(0, mine, batch)]
    n_chip = n_dp * n_tp // 2
    me_chip = dp * (n_tp // 2) + xx
    me = dp * n_tp + tp
    n_blk = n_dp * n_tp
    rows = x_ref.shape[0]
    cw = d_model // chunks

    def flip(v, bit):
        return 1 - v if bit else v

    def chip_peer(m):
        px = flip(xx, m & 1)
        pd = 2 * flip(lax.div(dp, 2), (m >> 2) & 1) + flip(lax.rem(dp, 2), (m >> 1) & 1)
        return pd, px

    peers = []
    for m in range(1, n_chip):
        pd, px = chip_peer(m)
        peers.append({"dp": pd, "tp": 2 * px + core})
    partner = {"dp": dp, "tp": 2 * xx + 1 - core}
    cross = {"dp": dp, "tp": 2 * (1 - xx) + 1 - core}

    def weights(b):
        e, n = batches[b]
        src = pl.ds(pl.multiple_of((base + e) * f_dim, f_dim), n * f_dim)
        s = b % ring
        return (pltpu.make_async_copy(wg.at[src], gbuf.at[s, pl.ds(0, n * f_dim)], gsem.at[s]),
                pltpu.make_async_copy(wu.at[src], ubuf.at[s, pl.ds(0, n * f_dim)], usem.at[s]))

    def down_weights(b):
        e, n = batches[b]
        src = pl.ds(pl.multiple_of((base + e) * f_dim, f_dim), n * f_dim)
        return pltpu.make_async_copy(wd.at[src], dbuf.at[pl.ds(e * f_dim, n * f_dim)], dsem.at[b])

    def start(b):
        for cp in weights(b):
            cp.start()

    barrier = pltpu.get_barrier_semaphore()
    for dev in peers + [partner, cross]:
        pl.semaphore_signal(barrier, inc=1, device_id=dev, device_id_type=MESH)
    loads = [pltpu.make_async_copy(a, b, lsem.at[i])
             for i, (a, b) in enumerate(((part_hbm, part), (x_hbm, x_ref), (g_hbm, g_ref),
                                     (picks_hbm, picks), (wr_hbm, wr)))]
    for cp in loads:
        cp.start()
    loads[0].wait()
    pl.semaphore_wait(barrier, len(peers) + 2)

    def block(t):
        return pl.ds(pl.multiple_of(t * 8, 8), 8)

    first = []
    for k in range(1, n_tp):
        t_to = lax.rem(tp + k, n_tp)
        cp = pltpu.make_async_remote_copy(
            src_ref=part.at[block(t_to)], dst_ref=recv1.at[k - 1],
            send_sem=s1.at[k - 1], recv_sem=r1.at[k - 1],
            device_id={"dp": dp, "tp": t_to}, device_id_type=MESH)
        cp.start()
        first.append(cp)

    for cp in loads[1:]:
        cp.wait()
    start(0)
    start(1)
    xf[...] = x_ref[...].astype(F32)
    pick_cols = []
    row8 = lax.broadcasted_iota(jnp.int32, (8, 128), 0)
    for kk in range(picks.shape[0]):
        pc = jnp.zeros((8, 128), jnp.int32)
        for i in range(8):
            pc = jnp.where(row8 == i, picks[kk, tp * 8 + i], pc)
        pick_cols.append(pc)

    for cp in first:
        cp.wait()
    attn_sum = part[block(tp), :]
    for k in range(1, n_tp):
        attn_sum = attn_sum + recv1[k - 1]
    x1 = (xf[block(tp), :] + attn_sum).astype(BF16).astype(F32)
    xf[block(tp), :] = x1
    h2 = norm_rows(x1, gain_row(g_ref))
    hall[me] = h2

    def wait_all(ref, sem):
        pltpu.make_async_copy(ref, ref, sem).wait()

    def spread(buf, i, m, ssem, rsem):
        return pltpu.make_async_remote_copy(
            src_ref=buf.at[i], dst_ref=buf.at[i], send_sem=ssem, recv_sem=rsem,
            device_id=peers[m], device_id_type=MESH)

    def relay(buf, i, m, ssem, rsem):
        return pltpu.make_async_remote_copy(
            src_ref=buf.at[i], dst_ref=buf.at[i], send_sem=ssem, recv_sem=rsem,
            device_id=partner, device_id_type=MESH)

    order = sorted(range(n_chip - 1), key=lambda m: -bin(m + 1).count("1"))
    hs = [spread(hall, me, m, s2.at[0], r2.at[m]) for m in range(n_chip - 1)]
    hd = [relay(hall, me, n_chip - 1, s3.at[0], r3.at[0])]
    for m in order:
        hs[m].start()
    hd[0].start()
    start(2)

    logits = lax.dot_general(h2, wr[...], NT, preferred_element_type=F32)
    lane = lax.broadcasted_iota(jnp.int32, (8, 128), 1)
    picked = []
    for pc in pick_cols:
        hit = (lane == pc)[:, :n_exp]
        picked.append(jnp.sum(jnp.where(hit, logits, 0.0), axis=1, keepdims=True))
    top = functools.reduce(jnp.maximum, picked)
    exs = [jnp.exp(p - top) for p in picked]
    den = functools.reduce(lambda a, b: a + b, exs)
    gates = jnp.zeros((8, 128), F32)
    for pc, ex in zip(pick_cols, exs):
        gates = gates + jnp.where(lane == pc, ex / den, 0.0)
    gall[me] = gates
    gs = [spread(gall, me, m, s4.at[0], r4.at[0]) for m in range(n_chip - 1)]
    gd = [relay(gall, me, n_chip - 1, s5.at[0], r5.at[0])]
    for m in order:
        gs[m].start()
    gd[0].start()

    def owner(m):
        pd, px = chip_peer(m + 1)
        return pd * n_tp + 2 * px + core

    for m in order:
        hs[m].wait_recv()
        cp = relay(hall, owner(m), m, s3.at[0], r3.at[0])
        cp.start()
        hd.append(cp)
    wait_all(hall.at[pl.ds(0, n_chip)], r3.at[0])

    for r in range(n_blk // 2):
        two = jnp.concatenate([hall[2 * r].astype(F32), hall[2 * r + 1].astype(F32)], axis=0)
        hb[16 * r:16 * r + 16, :] = two.astype(BF16)
    def products(b):
        s, width = b % ring, batches[b][1] * f_dim
        for cp in weights(b):
            cp.wait()
        gate = lax.dot_general(gbuf[s, :width], hb[...], NT, preferred_element_type=F32)
        up = lax.dot_general(ubuf[s, :width], hb[...], NT, preferred_element_type=F32)
        if b + ring < len(batches):
            start(b + ring)
        return gate, up

    def activate(b, gate, up):
        e0, n = batches[b]
        brow = lax.broadcasted_iota(jnp.int32, (128, n_blk * 8), 0)
        rows_g = [gt[pl.ds(base + e, 1), :] for e in range(e0, e0 + n)]
        for lo in range(0, n * f_dim, 128):
            hi = min(lo + 128, n * f_dim)
            ea, eb = lo // f_dim, (hi - 1) // f_dim
            grow = rows_g[ea]
            if eb > ea:
                grow = jnp.where(brow[:hi - lo] < eb * f_dim - lo, rows_g[ea], rows_g[eb])
            ga = gate[lo:hi]
            at = e0 * f_dim + lo
            zt = (grow * (ga * jax.nn.sigmoid(ga)) * up[lo:hi]).astype(BF16)
            z[:, at:at + hi - lo] = zt.T

    for b in range(len(batches)):
        down_weights(b).start()
    before = None
    for b in range(len(batches)):
        now = products(b)
        if b == 0:
            wait_all(gall.at[pl.ds(0, n_chip - 1)], r4.at[0])
            for m in order:
                cp = relay(gall, owner(m), m, s5.at[0], r5.at[0])
                cp.start()
                gd.append(cp)
        if b == 1:
            wait_all(gall.at[pl.ds(0, n_chip)], r5.at[0])
            gt[...] = gall[...].reshape(n_blk * 8, 128).T
        if before is not None:
            activate(b - 1, *before)
        before = now
    activate(len(batches) - 1, *before)
    for b in range(len(batches)):
        down_weights(b).wait()

    lag = 1
    finals = {}
    pair = {}

    def pair_sum(n):
        pair[n].wait_recv()
        psum[n] = acc[n, core] + drecv[n]
        for m in order:
            pd, px = chip_peer(m + 1)
            chip = pd * (n_tp // 2) + px
            cp = pltpu.make_async_remote_copy(
                src_ref=psum.at[n, block(chip)], dst_ref=frecv.at[n, m],
                send_sem=s7.at[0], recv_sem=r7.at[n], device_id=peers[m], device_id_type=MESH)
            cp.start()
            finals[n, m] = cp

    for n in range(chunks):
        cols = slice(n * cw, (n + 1) * cw)
        res = jnp.dot(z[...], dbuf[:, cols], preferred_element_type=F32)
        for j in range(n_chip):
            for q in range(2):
                at = (2 * j + q) * 8
                acc[n, q, 8 * j:8 * j + 8, :] = res[at:at + 8, :]
        cp = pltpu.make_async_remote_copy(
            src_ref=acc.at[n, 1 - core], dst_ref=drecv.at[n], send_sem=s6.at[0], recv_sem=r6.at[n],
            device_id=partner, device_id_type=MESH)
        cp.start()
        pair[n] = cp
        if n >= lag:
            pair_sum(n - lag)
    for n in range(chunks - lag, chunks):
        pair_sum(n)
    last, outs = [], []
    for n in range(chunks):
        total = psum[n, block(me_chip), :]
        wait_all(frecv.at[n], r7.at[n])
        for m in range(n_chip - 1):
            total = total + frecv[n, m]
        cols = slice(n * cw, (n + 1) * cw)
        yall[:, cols] = (xf[block(tp), cols] + total).astype(BF16)
        span = pl.ds(n * cw, cw)
        cp = pltpu.make_async_copy(yall.at[:, span], out_hbm.at[tp, :, span], osem.at[n])
        cp.start()
        outs.append(cp)
        for k in (2, 1, 3):
            t_to = lax.rem(tp + k, n_tp)
            cp = pltpu.make_async_remote_copy(
                src_ref=yall.at[:, span], dst_ref=out_hbm.at[tp, :, span],
                send_sem=s8.at[0], recv_sem=r8.at[0],
                device_id={"dp": dp, "tp": t_to}, device_id_type=MESH)
            cp.start()
            last.append(cp)
    wait_all(out_hbm.at[pl.ds(0, n_tp - 1)], r8.at[0])
    wait_all(hall.at[pl.ds(0, n_chip - 1)], s2.at[0])
    wait_all(hall.at[pl.ds(0, n_chip)], s3.at[0])
    wait_all(gall.at[pl.ds(0, n_chip - 1)], s4.at[0])
    wait_all(gall.at[pl.ds(0, n_chip)], s5.at[0])
    wait_all(drecv, s6.at[0])
    wait_all(frecv, s7.at[0])
    wait_all(hall.at[pl.ds(0, n_tp - 1)], s8.at[0])
    for cp in outs:
        cp.wait()


def experts(part, x, picks, g, wr, wg, wu, wd, n_dp, n_tp):
    rows, d_model = x.shape
    n_exp, f_dim, _ = wg.shape
    mine = n_exp // n_dp
    ring, batch, chunks = 3, 4, 4
    n_batch = -(-mine // batch)
    wg, wu, wd = (w.reshape(n_exp * f_dim, d_model) for w in (wg, wu, wd))
    n_chip = n_dp * n_tp // 2
    cw = d_model // chunks
    dma = pltpu.SemaphoreType.DMA
    out = pl.pallas_call(
        functools.partial(experts_kernel, n_dp=n_dp, n_tp=n_tp, n_exp=n_exp, ring=ring, batch=batch,
                          chunks=chunks),
        name="experts",
        out_shape=jax.ShapeDtypeStruct((n_tp, 8, d_model), BF16),
        in_specs=[ANY] * 8,
        out_specs=ANY,
        scratch_shapes=[
            pltpu.VMEM((rows, d_model), F32),
            pltpu.VMEM((rows, d_model), BF16),
            pltpu.VMEM((d_model // 128, 128), BF16),
            pltpu.SMEM(picks.shape, jnp.int32),
            pltpu.VMEM(wr.shape, BF16),
            dma((5,)), dma((chunks,)),
            pltpu.VMEM((ring, batch * f_dim, d_model), BF16),
            pltpu.VMEM((ring, batch * f_dim, d_model), BF16),
            pltpu.VMEM((mine * f_dim, d_model), BF16),
            pltpu.VMEM((rows, d_model), F32),
            pltpu.VMEM((n_tp - 1, 8, d_model), F32),
            pltpu.VMEM((n_dp * n_tp, 8, d_model), BF16),
            pltpu.VMEM((n_dp * n_tp * 8, d_model), BF16),
            pltpu.VMEM((n_dp * n_tp, 8, 128), F32),
            pltpu.VMEM((128, n_dp * n_tp * 8), F32),
            pltpu.VMEM((n_dp * n_tp * 8, mine * f_dim), BF16),
            pltpu.VMEM((chunks, 2, n_chip * 8, cw), F32),
            pltpu.VMEM((chunks, n_chip * 8, cw), F32),
            pltpu.VMEM((chunks, n_chip * 8, cw), F32),
            pltpu.VMEM((chunks, n_chip - 1, 8, cw), F32),
            pltpu.VMEM((8, d_model), BF16),
            dma((ring,)), dma((ring,)), dma((n_batch,)),
            dma((n_tp - 1,)), dma((n_tp - 1,)),
            dma((1,)), dma((n_chip - 1,)),
            dma((1,)), dma((1,)),
            dma((1,)), dma((1,)),
            dma((1,)), dma((1,)),
            dma((1,)), dma((chunks,)),
            dma((1,)), dma((chunks,)),
            dma((1,)), dma((1,)),
        ],
        compiler_params=pltpu.CompilerParams(
            collective_id=0, has_side_effects=True, vmem_limit_bytes=63 << 20),
        cost_estimate=pl.CostEstimate(flops=8_000_000_000, bytes_accessed=66_000_000, transcendentals=0),
    )(part, x, g.reshape(-1, 128), picks, wr, wg, wu, wd)
    return out.reshape(rows, d_model)


def solution(mesh):
    cache_spec = P("dp", None, "tp", None)
    in_specs = (P("dp", None), cache_spec, cache_spec, P("dp"), P("dp", None), P(None), P(None, "tp"), P(None, "tp"), P(None, "tp"), P("tp", None), P(None), P(None, None), P(None, None, "tp"), P(None, None, "tp"), P(None, "tp", None))
    out_specs = (P("dp", None), cache_spec, cache_spec)
    n_dp, n_tp = mesh.shape["dp"], mesh.shape["tp"]

    def layer_shard(hidden_in, k_cache, v_cache, seq_lens, chosen_experts, g_attn, w_q, w_k, w_v, w_o, g_moe, w_router, w_gate, w_up, w_down):
        rows, slots, heads, dim = k_cache.shape
        flat = (rows, slots * heads, dim)
        part, k_next, v_next = attention(
            hidden_in, k_cache.reshape(flat), v_cache.reshape(flat), seq_lens, g_attn, w_q, w_k, w_v, w_o)
        out = experts(part, hidden_in, chosen_experts.T, g_moe, w_router.T, w_gate.swapaxes(1, 2),
                      w_up.swapaxes(1, 2), w_down, n_dp, n_tp)
        return out, k_next.reshape(k_cache.shape), v_next.reshape(v_cache.shape)

    return jax.shard_map(layer_shard, mesh=mesh, in_specs=in_specs, out_specs=out_specs, check_vma=False)
```
